256 devices in a mesh: replica: 4 (over x, y), tp: 32 (over z), sub: 2 (over core).
Axes of the slice: x: 2, y: 2, z: 32, core: 2. Of those that a mesh axis runs over, the one named last changes fastest.
The devices are a block of a 4x8x32 slice.
Arguments:
- hidden_in: bfloat16 [16, 8192], P('replica'), parts along dimension 0, may hold values from -6 to 6
- norm_gain: float32 [32768], P('replica'), parts along dimension 0, may hold values from 0.1 to 1.9
- wqkv_old: bfloat16 [128, 2, 1280, 1024], P(('replica', 'tp'), 'sub'), parts along dimension 0, may hold values from -0.1875 to 0.1875
- wo: bfloat16 [32768, 8192], P(('replica', 'tp', 'sub')), parts along dimension 0, may hold values from -0.0625 to 0.0625
- key_cache: bfloat16 [16, 4096, 1024], P('replica', ('tp', 'sub')), parts along dimension 0, may hold values from -240 to 240
- value_cache: bfloat16 [16, 4096, 1024], P('replica', ('tp', 'sub')), parts along dimension 0, may hold values from -6 to 6
- lengths: int32 [16], P('replica'), parts along dimension 0, may hold values from 1 to 4096
- section_order: int32 [64], P('replica'), parts along dimension 0, may hold values from 0 to 15, each once
Outputs:
- mixed_out: bfloat16 [16, 8192], P('replica'), parts along dimension 0
- wqkv_new: bfloat16 [128, 2, 160, 8192], P(('replica', 'tp'), 'sub'), parts along dimension 0
The draws below stay inside these ranges and needn't reach their ends.
There are 4 independent parts, one for each index of `replica`. The reference program is written for one: setup_inputs(seed, part) draws one part's arguments, and reference() takes and returns one part's arrays. A program takes and returns all parts, laid end to end along the dimension named above; each array names one. Nothing has to cross between parts.
Inputs may be any that keep to these rules, and one draw needn't show every extreme that they name: `section_order`: each input row block appears once. The new token's position is lengths[b].
All inputs are finite; a program needn't handle non-finite values.
Results may differ from the reference program's by a relative error of at most 0.0085.
The reference program's roundings to bfloat16 on the way (of `full_t`, `normed`, `projected` and `attended`) count: a program that leaves them out, or rounds other values in their place, can miss the bound.
Values may be sent and summed in bfloat16 or wider, within the bound.
A program may use at most 64 MiB of HBM per device.

```python
import math
import jax
import jax.numpy as jnp
from jax import lax

D = 8192
HEADS = 64
KV_HEADS = 8
HEAD_DIM = 128
RANKS = 8
ROW_BLOCKS = 16
SEQS = 4
CACHE_LEN = 4096
QKV = 10240
RANK_COLS = 1280
COLS_DEV = 160
ROWS_OLD = 1024
BLOCK_ROWS = 512
N_TP = 32


def draw_key_cache(key, part):
    base = jax.random.normal(jax.random.fold_in(key, 11), (SEQS, CACHE_LEN, KV_HEADS * HEAD_DIM), jnp.float32)
    return jnp.clip(base, -6.0, 6.0).astype(jnp.bfloat16)


def place_ends(entries, key, smallest, top_value):
    spot = [jax.random.randint(jax.random.fold_in(key, axis), (), 0, length) for axis, length in enumerate(entries.shape)]
    widest = entries.shape.index(max(entries.shape))
    neighbour = spot[:widest] + [(spot[widest] + 1) % entries.shape[widest]] + spot[widest + 1:]
    return entries.at[tuple(spot)].set(smallest).at[tuple(neighbour)].set(top_value)


def level_of(key, extent, split, smallest, high):
    gain = 1.0
    for dim, shards_of in split:
        steps = jax.random.uniform(jax.random.fold_in(jax.random.fold_in(key, 6), dim), (shards_of,), jnp.float32, smallest / len(split), high / len(split))
        gain = gain * jnp.repeat(jnp.exp(steps), extent[dim] // shards_of).reshape((-1,) + (1,) * (len(extent) - 1 - dim))
    return gain


def normal_values(own_key, shape, scale, limit, pieces=(), kind=jnp.bfloat16):
    array = scale * jax.random.normal(own_key, shape, jnp.float32)
    if pieces:
        array = array * level_of(own_key, shape, pieces, -0.22, 0.18)
    return jnp.clip(array, -limit, limit).astype(kind)


def setup_inputs(seed: int = 0, part: int = 0) -> dict:
    seeds = jax.random.split(jax.random.key(seed), 9)
    part_keys = jax.random.split(jax.random.fold_in(seeds[8], part), 9)
    return {
        "hidden_in": normal_values(part_keys[0], (SEQS, D), 1.0, 6.0),
        "norm_gain": jnp.clip(1.0 + 0.18 * jax.random.normal(part_keys[1], (D,), jnp.float32), 0.1, 1.9),
        "wqkv_old": normal_values(part_keys[2], (N_TP, 2, RANK_COLS, ROWS_OLD), (D // 9) ** -0.5, 0.1875, ((0, 32), (1, 2))),
        "wo": normal_values(part_keys[3], (HEADS * HEAD_DIM, D), (HEADS * HEAD_DIM) ** -0.5, 0.0625, ((0, 64),)),
        "key_cache": draw_key_cache(jax.random.fold_in(jax.random.fold_in(seeds[8], part), 71), part),
        "value_cache": normal_values(part_keys[5], (SEQS, CACHE_LEN, KV_HEADS * HEAD_DIM), 1.0, 6.0, ((1, 64),)),
        "lengths": place_ends(jax.random.randint(part_keys[6], (SEQS,), 1, CACHE_LEN + 1), jax.random.fold_in(part_keys[6], 1), 1, CACHE_LEN).astype(jnp.int32),
        "section_order": jax.random.permutation(part_keys[7], ROW_BLOCKS).astype(jnp.int32),
    }


def rotary(values, positions):
    half = values.shape[-1] // 2
    freqs = 500000.0 ** (-jnp.arange(half, dtype=jnp.float32) * 2.0 / values.shape[-1])
    angles = positions.astype(jnp.float32)[:, None] * freqs[None, :]
    cosine = jnp.cos(angles)[:, None, :]
    sine = jnp.sin(angles)[:, None, :]
    first_half = values[..., :half]
    second_half = values[..., half:]
    return jnp.concatenate([first_half * cosine - second_half * sine, second_half * cosine + first_half * sine], -1)

def rms_normed(hidden_in, norm_gain):
    widened = hidden_in.astype(jnp.float32)
    factor = lax.rsqrt(lax.optimization_barrier(jnp.mean(widened * widened, -1, keepdims=True)) + 1e-05)
    return (widened, (widened * factor * norm_gain).astype(jnp.bfloat16))

def reference(hidden_in, norm_gain, wqkv_old, wo, key_cache, value_cache, lengths, section_order):
    section_count = N_TP // 4
    per_section = ROW_BLOCKS // section_count
    groups = HEADS // KV_HEADS
    q_width = HEADS * HEAD_DIM
    kv_width = KV_HEADS * HEAD_DIM
    by_rank = wqkv_old.reshape(section_count, RANKS, RANK_COLS, per_section, BLOCK_ROWS)
    blocks = jnp.transpose(by_rank, (0, 3, 1, 2, 4)).reshape(ROW_BLOCKS, RANKS, RANK_COLS, BLOCK_ROWS)
    ordered = jnp.zeros_like(blocks).at[section_order].set(blocks)
    full_t = jnp.transpose(ordered, (1, 2, 0, 3)).reshape(QKV, D)
    wqkv_new = jnp.transpose(full_t.reshape(4, 2, section_count, COLS_DEV, D), (2, 0, 1, 3, 4)).reshape(N_TP, 2, COLS_DEV, D)
    widened, normed = rms_normed(hidden_in, norm_gain)
    projected = lax.dot_general(normed, full_t, (((1,), (1,)), ((), ())), preferred_element_type=jnp.float32).astype(jnp.bfloat16)
    queries = rotary(projected[:, :q_width].astype(jnp.float32).reshape(SEQS, HEADS, HEAD_DIM), lengths).astype(jnp.bfloat16)
    new_keys = rotary(projected[:, q_width:q_width + kv_width].astype(jnp.float32).reshape(SEQS, KV_HEADS, HEAD_DIM), lengths).astype(jnp.bfloat16)
    new_values = projected[:, q_width + kv_width:].astype(jnp.float32).reshape(SEQS, KV_HEADS, HEAD_DIM)
    grouped = queries.astype(jnp.float32).reshape(SEQS, KV_HEADS, groups, HEAD_DIM)
    keys_all = key_cache.astype(jnp.float32).reshape(SEQS, CACHE_LEN, KV_HEADS, HEAD_DIM)
    values_all = value_cache.astype(jnp.float32).reshape(SEQS, CACHE_LEN, KV_HEADS, HEAD_DIM)
    inverse = 1.0 / math.sqrt(HEAD_DIM)
    scores = jnp.einsum('bkgd,bpkd->bkgp', grouped, keys_all) * inverse
    usable = (jnp.arange(CACHE_LEN, dtype=jnp.int32)[None, :] < lengths[:, None])[:, None, None, :]
    own_score = lax.optimization_barrier(jnp.sum(grouped * new_keys.astype(jnp.float32)[:, :, None, :], -1)) * inverse
    highest = jnp.maximum(lax.optimization_barrier(jnp.max(jnp.where(usable, scores, -1e+30), -1)), own_score)
    weights = jnp.exp(jnp.where(usable, scores - highest[..., None], -1e+30))
    own_weight = jnp.exp(own_score - highest)
    total = lax.optimization_barrier(jnp.sum(weights, -1)) + own_weight
    mixture = jnp.einsum('bkgp,bpkd->bkgd', weights, values_all) + own_weight[..., None] * new_values[:, :, None, :]
    attended = (mixture / total[..., None]).reshape(SEQS, q_width).astype(jnp.bfloat16)
    mixed_out = (widened + jnp.dot(attended, wo, preferred_element_type=jnp.float32)).astype(jnp.bfloat16)
    return (mixed_out, wqkv_new)
```

```python
import functools
import math

import jax
import jax.numpy as jnp
from jax import lax
from jax.experimental import pallas as pl
from jax.experimental.pallas import tpu as pltpu
from jax.sharding import PartitionSpec as P

HEADS = 64
KV_HEADS = 8
HEAD_DIM = 128
ROW_BLOCKS = 16
NEAR = 4
SECTIONS = 8
STEP_ROWS = 8

MESH = pl.DeviceIdType.MESH
F32 = jnp.float32
BF16 = jnp.bfloat16


def nt_dot(x, y):
    return lax.dot_general(x, y, (((1,), (1,)), ((), ())), preferred_element_type=F32)


def split_stat(stat):
    low = lax.broadcasted_iota(jnp.int32, stat.shape, stat.ndim - 1) < 64
    turned = pltpu.roll(stat, 64, stat.ndim - 1)
    return jnp.where(low, stat, turned), jnp.where(low, turned, stat)


def merged(parts):
    best = parts[0][1]
    for _, top, _ in parts[1:]:
        best = jnp.maximum(best, top)
    mix, total = None, None
    for m, top, s in parts:
        f = jnp.exp(top - best)
        mix = m * f if mix is None else mix + m * f
        total = s * f if total is None else total + s * f
    return mix, best, total


def joined_stat(best, total):
    low = lax.broadcasted_iota(jnp.int32, best.shape, best.ndim - 1) < 64
    return jnp.where(low, best, total)


def main_kernel(
    hid, gain, turn, lengths, order, w, wo, kc, vc,
    recv, g_out,
    w_v, wo_v, k_v, v_v, nrm, p_tx, p_rx, q_tx, q_all, rows, state, a_rx1, a_rx2, a_tx, a_rx3,
    part, o_rx1, o_rx2, o_tx, o_rx3, g_all,
    load_sem, big_s, big_r, far_s, far_r, loc_s, loc_r, duo_s, duo_r, known_lo, known_hi,
):
    count = lax.axis_size("tp")
    t = lax.axis_index("tp")
    s = lax.axis_index("sub")
    a = t // NEAR
    c = t % NEAR
    seqs, width = hid.shape
    cols = recv.shape[1]

    def far_id(k):
        return {"tp": lax.rem(t + NEAR * k, count)}

    def loc_id(m):
        return {"tp": NEAR * a + lax.rem(c + m, NEAR)}

    duo_id = {"sub": 1 - s}

    barrier = pltpu.get_barrier_semaphore()
    greeted = [far_id(1), far_id(SECTIONS - 1), loc_id(1), loc_id(2), loc_id(3), duo_id]
    for target in greeted:
        pl.semaphore_signal(barrier, inc=1, device_id=target, device_id_type=MESH)

    loads = [
        pltpu.make_async_copy(src, dst, load_sem.at[i])
        for i, (src, dst) in enumerate(((w, w_v), (kc, k_v), (vc, v_v), (wo, wo_v)))
    ]
    loads[0].start()
    pl.semaphore_wait(barrier, len(greeted))

    sent = dict.fromkeys(range(1, SECTIONS), 0)

    def piece(k, row, height):
        b = lax.rem(a + k, SECTIONS)
        first = pl.multiple_of(b * cols + row, 8)
        return pltpu.make_async_remote_copy(
            src_ref=w.at[pl.ds(first, height), :],
            dst_ref=recv.at[a, pl.ds(row, height), :],
            send_sem=big_s.at[k],
            recv_sem=big_r.at[SECTIONS - k],
            device_id=far_id(k),
            device_id_type=MESH,
        )

    def stream(ks, n):
        ks = [k for k in ks if sent[k] < cols]
        n = min([n] + [(cols - sent[k]) // STEP_ROWS for k in ks])
        if not ks or n == 0:
            return
        starts = {k: sent[k] for k in ks}

        def body(i, carry):
            for k in ks:
                piece(k, pl.multiple_of(starts[k] + i * STEP_ROWS, 8), STEP_ROWS).start()
            return carry

        lax.fori_loop(0, n, body, 0)
        for k in ks:
            sent[k] += n * STEP_ROWS

    everyone = (1, 7, 2, 6, 3, 5, 4)

    def tell(stage):
        pl.semaphore_signal(known_lo.at[stage], inc=1, device_id=far_id(1), device_id_type=MESH)
        pl.semaphore_signal(
            known_hi.at[stage], inc=1, device_id=far_id(SECTIONS - 1), device_id_type=MESH
        )

    def hear(stage):
        pl.semaphore_wait(known_lo.at[stage], 1)
        pl.semaphore_wait(known_hi.at[stage], 1)

    tell(0)
    stream((1, 7), 8)
    for copy in loads[1:]:
        copy.start()
    hear(0)
    tell(1)
    stream((2, 6), 2)

    def far_copies(phase, src, dst):
        out = []
        for k in range(1, SECTIONS):
            out.append(
                pltpu.make_async_remote_copy(
                    src_ref=src(lax.rem(a + k, SECTIONS)),
                    dst_ref=dst,
                    send_sem=far_s.at[phase, k],
                    recv_sem=far_r.at[phase, SECTIONS - k],
                    device_id=far_id(k),
                    device_id_type=MESH,
                )
            )
        return out

    def loc_copies(phase, src, dst):
        out = []
        for m in range(1, NEAR):
            out.append(
                pltpu.make_async_remote_copy(
                    src_ref=src(lax.rem(c + m, NEAR)),
                    dst_ref=dst,
                    send_sem=loc_s.at[phase, m],
                    recv_sem=loc_r.at[phase, NEAR - m],
                    device_id=loc_id(m),
                    device_id_type=MESH,
                )
            )
        return out

    def duo_copies(phase, src, dst):
        return [
            pltpu.make_async_remote_copy(
                src_ref=src,
                dst_ref=dst,
                send_sem=duo_s.at[phase],
                recv_sem=duo_r.at[phase],
                device_id=duo_id,
                device_id_type=MESH,
            )
        ]

    def start(copies):
        for copy in copies:
            copy.start()

    def wait(copies):
        for copy in copies:
            copy.wait()

    block = nrm.shape[2]
    squares = jnp.zeros((seqs, 1), F32)
    for i in range(ROW_BLOCKS):
        x = hid[:, i * block : (i + 1) * block].astype(F32)
        squares = squares + jnp.sum(x * x, -1, keepdims=True)
    factor = lax.rsqrt(squares * (1.0 / width) + 1e-05)
    for i in range(ROW_BLOCKS):
        x = hid[:, i * block : (i + 1) * block].astype(F32)
        y = (x * factor * gain[:, i * block : (i + 1) * block]).astype(BF16)
        nrm[i] = y.astype(F32)

    hear(1)
    tell(2)
    stream((3, 5), 1)

    per_section = ROW_BLOCKS // SECTIONS
    mine = [nrm[order[per_section * a + i]].astype(BF16) for i in range(per_section)]
    normed = jnp.concatenate(mine, -1)
    loads[0].wait()
    units = w.shape[0] // HEAD_DIM
    half = units // 2
    for u in range(units):
        y = nt_dot(normed, w_v[u * HEAD_DIM : (u + 1) * HEAD_DIM, :])
        for b in range(seqs):
            p_tx[2 * b + u // half, u % half : u % half + 1, :] = y[b : b + 1, :]
    own_rows = pl.ds(pl.multiple_of(a * cols, 8), cols)
    keep = pltpu.make_async_copy(w_v.at[own_rows, :], recv.at[a], load_sem.at[4])
    keep.start()

    hear(2)
    copies = far_copies(0, lambda b: p_tx.at[b], p_rx.at[a])
    start(copies)
    stream(everyone, 1)
    p_rx[a] = p_tx[a]
    wait(copies)
    total = p_rx[0]
    for i in range(1, SECTIONS):
        total = total + p_rx[i]
    q_tx[...] = total.astype(BF16)
    q_all[s, c, a] = total.astype(BF16)

    copies = far_copies(1, lambda b: q_tx, q_all.at[s, c, a])
    start(copies)
    stream(everyone, 1)
    wait(copies)

    copies = loc_copies(0, lambda b: q_all.at[s, c], q_all.at[s, c])
    start(copies)
    stream(everyone, 1)
    wait(copies)

    copies = duo_copies(0, q_all.at[s], q_all.at[s])
    start(copies)
    wait(copies)

    rotated = HEADS + KV_HEADS
    for b in range(seqs):
        for j in range(2 * SECTIONS):
            rank = j // 2
            rows[b, j * half : (j + 1) * half, :] = q_all[rank % 2, rank // 2, 2 * b + j % 2][
                :half
            ].astype(F32)
        x = rows[b, :rotated, :]
        x = x * turn[b, 0:1, :] + pltpu.roll(x, 64, 1) * turn[b, 1:2, :]
        rows[b, :rotated, :] = x.astype(BF16).astype(F32)

    for copy in loads[1:3]:
        copy.wait()
    groups = HEADS // KV_HEADS
    inverse = 1.0 / math.sqrt(HEAD_DIM)
    pos_count = k_v.shape[1]
    first = (2 * t + s) * pos_count

    def one_sequence(b, carry):
        position = first + lax.broadcasted_iota(jnp.int32, (groups, pos_count), 1)
        usable = position < lengths[b]
        low = lax.broadcasted_iota(jnp.int32, (groups, HEAD_DIM), 1) < 64
        for k in range(KV_HEADS):
            lanes = slice(k * HEAD_DIM, (k + 1) * HEAD_DIM)
            q = rows[b, k * groups : (k + 1) * groups, :].astype(BF16)
            scores = nt_dot(q, k_v[b, :, lanes]) * inverse
            top = jnp.max(jnp.where(usable, scores, -1e30), -1, keepdims=True)
            weights = jnp.exp(jnp.where(usable, scores - top, -1e30))
            total = jnp.sum(weights, -1, keepdims=True)
            mix = jnp.dot(weights.astype(BF16), v_v[b, :, lanes], preferred_element_type=F32)
            stat = jnp.where(low, top, total)
            for g in range(groups):
                state[g % 2, g // 2, k, pl.ds(b, 1), :] = mix[g : g + 1, :]
                state[g % 2, g // 2, k, pl.ds(seqs + b, 1), :] = stat[g : g + 1, :]
        return carry

    lax.fori_loop(0, seqs, one_sequence, 0)

    def parted(ref):
        mix = ref[0:seqs, :]
        top, total = split_stat(ref[seqs : 2 * seqs, :])
        return mix, top, total

    def put(ref, part):
        mix, best, total = part
        ref[0:seqs, :] = mix
        ref[seqs : 2 * seqs, :] = joined_stat(best, total)

    copies = duo_copies(1, state.at[1 - s], a_rx1)
    start(copies)
    wait(copies)

    def merge_duo(i, carry):
        u, v = i // SECTIONS, i % SECTIONS
        put(a_tx.at[u, v], merged([parted(state.at[s, u, v]), parted(a_rx1.at[u, v])]))
        return carry

    lax.fori_loop(0, NEAR * SECTIONS, merge_duo, 0)

    copies = loc_copies(1, lambda m: a_tx.at[m], a_rx2.at[c])
    start(copies)
    stream(everyone, 1)
    a_rx2[c] = a_tx[c]
    wait(copies)

    def merge_loc(v, carry):
        put(state.at[0, 0, v], merged([parted(a_rx2.at[i, v]) for i in range(NEAR)]))
        return carry

    lax.fori_loop(0, SECTIONS, merge_loc, 0)

    copies = far_copies(2, lambda b: state.at[0, 0, b], a_rx3.at[a])
    start(copies)
    stream(everyone, 1)
    a_rx3[a] = state[0, 0, a]
    wait(copies)
    mix, best, total = merged([parted(a_rx3.at[i]) for i in range(SECTIONS)])

    head = groups * a + 2 * c + s

    def head_rows(at):
        return jnp.concatenate([rows[b, pl.ds(at, 1), :] for b in range(seqs)], 0)

    own_score = jnp.sum(head_rows(head) * head_rows(HEADS + a), -1, keepdims=True) * inverse
    highest = jnp.maximum(best, own_score)
    old_scale = jnp.exp(best - highest)
    own_weight = jnp.exp(own_score - highest)
    numerator = mix * old_scale + own_weight * head_rows(rotated + a)
    denominator = total * old_scale + own_weight
    attended = (numerator / denominator).astype(BF16)

    loads[3].wait()
    wide = 512
    for i in range(width // wide):
        y = jnp.dot(attended, wo_v[:, i * wide : (i + 1) * wide], preferred_element_type=F32)
        for j in range(wide // 128):
            part[i * (wide // 128) + j] = y[:, j * 128 : (j + 1) * 128]

    half_blocks = part.shape[0] // 2
    own_half = pl.ds(s * half_blocks, half_blocks)
    copies = duo_copies(2, part.at[pl.ds((1 - s) * half_blocks, half_blocks)], o_rx1)
    start(copies)
    wait(copies)
    part[own_half] = part[own_half] + o_rx1[...]

    def quarter(m):
        return part.at[pl.ds(s * half_blocks + m * SECTIONS, SECTIONS)]

    copies = loc_copies(2, quarter, o_rx2.at[c])
    start(copies)
    stream(everyone, 1)
    o_rx2[c] = part[pl.ds(s * half_blocks + c * SECTIONS, SECTIONS)]
    wait(copies)
    o_tx[...] = (o_rx2[0] + o_rx2[1]) + (o_rx2[2] + o_rx2[3])

    copies = far_copies(3, lambda b: o_tx.at[b], o_rx3.at[a])
    start(copies)
    stream(everyone, 1)
    o_rx3[a] = o_tx[a]
    wait(copies)
    total = o_rx3[0]
    for i in range(1, SECTIONS):
        total = total + o_rx3[i]
    col = pl.multiple_of((s * half_blocks + c * SECTIONS + a) * 128, 128)
    g_all[s, c, a] = (hid[:, pl.ds(col, 128)].astype(F32) + total).astype(BF16)

    copies = far_copies(4, lambda b: g_all.at[s, c, a], g_all.at[s, c, a])
    start(copies)
    stream(everyone, 1)
    wait(copies)

    copies = loc_copies(3, lambda m: g_all.at[s, c], g_all.at[s, c])
    start(copies)
    stream(everyone, 1)
    wait(copies)

    copies = duo_copies(3, g_all.at[s], g_all.at[s])
    start(copies)
    while any(sent[k] < cols for k in everyone):
        stream(everyone, 1)
    wait(copies)
    give = pltpu.make_async_copy(g_all, g_out, load_sem.at[5])
    give.start()
    keep.wait()
    give.wait()
    for k in everyone:
        piece(k, 0, cols).wait()


def place_kernel(order, recv, g_in, mixed, new, buf, in_sem, out_sem):
    block = buf.shape[2]
    per_section = ROW_BLOCKS // SECTIONS
    reads = []
    for i in range(ROW_BLOCKS):
        src = recv.at[i // per_section, :, pl.ds((i % per_section) * block, block)]
        copy = pltpu.make_async_copy(src, buf.at[i], in_sem.at[i])
        copy.start()
        reads.append(copy)
    blocks = g_in.shape[0] * g_in.shape[1] * g_in.shape[2]
    for j in range(blocks):
        mixed[:, j * 128 : (j + 1) * 128] = g_in[
            j // (NEAR * SECTIONS), (j // SECTIONS) % NEAR, j % SECTIONS
        ]
    writes = []
    for i in range(ROW_BLOCKS):
        reads[i].wait()
        at = pl.multiple_of(order[i] * block, 128)
        copy = pltpu.make_async_copy(buf.at[i], new.at[:, pl.ds(at, block)], out_sem.at[i])
        copy.start()
        writes.append(copy)
    for copy in writes:
        copy.wait()


def shards(hidden_in, norm_gain, wqkv_old, wo, key_cache, value_cache, lengths, section_order):
    seqs, width = hidden_in.shape
    _, _, rank_cols, rows_old = wqkv_old.shape
    cols = rank_cols // SECTIONS
    block = width // ROW_BLOCKS
    pos_count = key_cache.shape[1]

    half_dim = HEAD_DIM // 2
    freqs = 500000.0 ** (-jnp.arange(half_dim, dtype=F32) * 2.0 / HEAD_DIM)
    angles = lengths.astype(F32)[:, None] * freqs[None, :]
    cosine, sine = jnp.cos(angles), jnp.sin(angles)
    turn = jnp.stack(
        [jnp.concatenate([cosine, cosine], -1), jnp.concatenate([-sine, sine], -1)], 1
    )

    vmem = pl.BlockSpec(memory_space=pltpu.VMEM)
    smem = pl.BlockSpec(memory_space=pltpu.SMEM)
    hbm = pl.BlockSpec(memory_space=pl.ANY)
    dma = pltpu.SemaphoreType.DMA
    tile = (8, 128)
    recv, g_out = pl.pallas_call(
        main_kernel,
        name="stream_and_decode",
        out_shape=(
            jax.ShapeDtypeStruct((SECTIONS, cols, rows_old), BF16),
            jax.ShapeDtypeStruct((2, NEAR, SECTIONS, seqs, 128), BF16),
        ),
        in_specs=[vmem, vmem, vmem, smem, smem, hbm, hbm, hbm, hbm],
        out_specs=(hbm, hbm),
        scratch_shapes=[
            pltpu.VMEM((rank_cols, rows_old), BF16),
            pltpu.VMEM(wo.shape, BF16),
            pltpu.VMEM(key_cache.shape, BF16),
            pltpu.VMEM(value_cache.shape, BF16),
            pltpu.VMEM((ROW_BLOCKS, seqs, block), F32),
            pltpu.VMEM((SECTIONS, *tile), F32),
            pltpu.VMEM((SECTIONS, *tile), F32),
            pltpu.VMEM(tile, BF16),
            pltpu.VMEM((2, NEAR, SECTIONS, *tile), BF16),
            pltpu.VMEM((seqs, HEADS + 2 * KV_HEADS, HEAD_DIM), F32),
            pltpu.VMEM((2, NEAR, SECTIONS, *tile), F32),
            pltpu.VMEM((NEAR, SECTIONS, *tile), F32),
            pltpu.VMEM((NEAR, SECTIONS, *tile), F32),
            pltpu.VMEM((NEAR, SECTIONS, *tile), F32),
            pltpu.VMEM((SECTIONS, *tile), F32),
            pltpu.VMEM((width // 128, seqs, 128), F32),
            pltpu.VMEM((width // 256, seqs, 128), F32),
            pltpu.VMEM((NEAR, SECTIONS, seqs, 128), F32),
            pltpu.VMEM((SECTIONS, seqs, 128), F32),
            pltpu.VMEM((SECTIONS, seqs, 128), F32),
            pltpu.VMEM((2, NEAR, SECTIONS, seqs, 128), BF16),
            dma((6,)),
            dma((SECTIONS,)),
            dma((SECTIONS,)),
            dma((5, SECTIONS)),
            dma((5, SECTIONS)),
            dma((4, NEAR)),
            dma((4, NEAR)),
            dma((4,)),
            dma((4,)),
            pltpu.SemaphoreType.REGULAR((3,)),
            pltpu.SemaphoreType.REGULAR((3,)),
        ],
        compiler_params=pltpu.CompilerParams(collective_id=0, has_side_effects=True),
    )(
        hidden_in,
        norm_gain.reshape(1, width),
        turn,
        lengths,
        section_order,
        wqkv_old.reshape(rank_cols, rows_old),
        wo,
        key_cache,
        value_cache,
    )

    mixed_out, new_weight = pl.pallas_call(
        place_kernel,
        name="place",
        out_shape=(
            jax.ShapeDtypeStruct((seqs, width), BF16),
            jax.ShapeDtypeStruct((cols, width), BF16),
        ),
        in_specs=[smem, hbm, vmem],
        out_specs=(vmem, hbm),
        scratch_shapes=[
            pltpu.VMEM((ROW_BLOCKS, cols, block), BF16),
            dma((ROW_BLOCKS,)),
            dma((ROW_BLOCKS,)),
        ],
    )(section_order, recv, g_out)
    return mixed_out, new_weight[None, None]


def solution(mesh):
    placed = (
        P("replica", None),
        P("replica"),
        P(("replica", "tp"), "sub", None, None),
        P(("replica", "tp", "sub"), None),
        P("replica", ("tp", "sub"), None),
        P("replica", ("tp", "sub"), None),
        P("replica"),
        P("replica"),
    )
    return jax.shard_map(
        shards,
        mesh=mesh,
        in_specs=placed,
        out_specs=(P("replica", None), P(("replica", "tp"), "sub", None, None)),
        check_vma=False,
    )
```

```python
import functools
import math

import jax
import jax.numpy as jnp
import numpy as np
from jax import lax
from jax.experimental import pallas as pl
from jax.experimental.pallas import tpu as pltpu
from jax.sharding import PartitionSpec as P

HEADS = 64
KV_HEADS = 8
HEAD_DIM = 128
ROW_BLOCKS = 16
NEAR = 4
SECTIONS = 8
HIGH_ROWS = 72
STEP_ROWS = 8

FEEDS = (4, 4, 7, 2, 4, 3, 4, 4, 4)
MESH = pl.DeviceIdType.MESH
F32 = jnp.float32
BF16 = jnp.bfloat16


def nt_dot(x, y):
    return lax.dot_general(x, y, (((1,), (1,)), ((), ())), preferred_element_type=F32)


def spread(x):
    lane = lax.broadcasted_iota(jnp.int32, x.shape, 1)
    row = lax.broadcasted_iota(jnp.int32, x.shape, 0)
    return jnp.max(jnp.where((lane >> 5) == row, x, -3e38), -1, keepdims=True)


def merged(tiles, seqs):
    tops, totals = [], []
    low = (lax.broadcasted_iota(jnp.int32, (seqs, 128), 1) & 16) == 0
    for tile in tiles:
        stat = jnp.broadcast_to(tile[seqs : seqs + 1, :], (seqs, 128))
        tops.append(jnp.where(low, stat, pltpu.roll(stat, 16, 1)))
        totals.append(jnp.where(low, pltpu.roll(stat, 112, 1), stat))
    best = functools.reduce(jnp.maximum, tops)
    mix, total = None, None
    for tile, top, s in zip(tiles, tops, totals):
        f = jnp.exp(top - best)
        m = tile[0:seqs, :] * spread(f)
        mix = m if mix is None else mix + m
        total = s * f if total is None else total + s * f
    return mix, best, total


def main_kernel(
    hid_in, gain_in, table_in, lengths, order, w, wo, kc, vc,
    recv, g_out,
    hid, gain, table, w_v, wo_v, k_v, v_v, nrm, p_tx, p_rx, q_tx, q_all, rows, state, a_rx1, a_rx2, a_tx, a_rx3,
    part, o_rx1, o_rx2, o_tx, o_rx3, g_all,
    load_sem, big_s, big_r, far_s, far_r, loc_s, loc_r, duo_s, duo_r, known_lo, known_hi,
):
    count = lax.axis_size("tp")
    t = lax.axis_index("tp")
    s = lax.axis_index("sub")
    a = t // NEAR
    c = t % NEAR
    seqs, width = hid_in.shape
    cols = recv.shape[1]

    def far_id(k):
        return {"tp": lax.rem(t + NEAR * k, count)}

    def loc_id(m):
        return {"tp": NEAR * a + lax.rem(c + m, NEAR)}

    duo_id = {"sub": 1 - s}

    barrier = pltpu.get_barrier_semaphore()
    greeted = [far_id(1), far_id(SECTIONS - 1), loc_id(1), loc_id(2), loc_id(3), duo_id]
    for target in greeted:
        pl.semaphore_signal(barrier, inc=1, device_id=target, device_id_type=MESH)

    loads = [
        pltpu.make_async_copy(src, dst, load_sem.at[i])
        for i, (src, dst) in enumerate(
            (
                (w, w_v),
                (kc, k_v),
                (vc, v_v),
                (wo, wo_v),
                (hid_in, hid),
                (gain_in, gain),
                (table_in, table),
            )
        )
    ]
    for i in (4, 5, 0):
        loads[i].start()
    pl.semaphore_wait(barrier, len(greeted))

    sent = dict.fromkeys(range(1, SECTIONS), 0)

    def piece(k, row, height):
        b = lax.rem(a + k, SECTIONS)
        first = pl.multiple_of(b * cols + row, 8)
        return pltpu.make_async_remote_copy(
            src_ref=w.at[pl.ds(first, height), :],
            dst_ref=recv.at[a, pl.ds(row, height), :],
            send_sem=big_s.at[k],
            recv_sem=big_r.at[SECTIONS - k],
            device_id=far_id(k),
            device_id_type=MESH,
        )

    def stream(ks, n):
        ks = [k for k in ks if sent[k] < cols]
        n = min([n] + [(cols - sent[k]) // STEP_ROWS for k in ks])
        if not ks or n == 0:
            return
        starts = {k: sent[k] for k in ks}

        def body(i, carry):
            for k in ks:
                piece(k, pl.multiple_of(starts[k] + i * STEP_ROWS, 8), STEP_ROWS).start()
            return carry

        lax.fori_loop(0, n, body, 0)
        for k in ks:
            sent[k] += n * STEP_ROWS

    everyone = (1, 7, 2, 6, 3, 5, 4)
    halves = ((1, 7, 3, 5), (2, 6, 4))
    turns = [0]

    def feed(n):
        for _ in range(n):
            stream(halves[turns[0] % 2], 1)
            turns[0] += 1

    feeds = iter(FEEDS)

    def tell(stage):
        pl.semaphore_signal(known_lo.at[stage], inc=1, device_id=far_id(1), device_id_type=MESH)
        pl.semaphore_signal(
            known_hi.at[stage], inc=1, device_id=far_id(SECTIONS - 1), device_id_type=MESH
        )

    def hear(stage):
        pl.semaphore_wait(known_lo.at[stage], 1)
        pl.semaphore_wait(known_hi.at[stage], 1)

    tell(0)
    stream((1, 7), 12)
    for i in (6, 1, 2, 3):
        loads[i].start()
    hear(0)
    tell(1)
    stream((2, 6), 4)

    def far_copies(phase, src, dst):
        out = []
        for k in range(1, SECTIONS):
            out.append(
                pltpu.make_async_remote_copy(
                    src_ref=src(lax.rem(a + k, SECTIONS)),
                    dst_ref=dst,
                    send_sem=far_s.at[phase, k],
                    recv_sem=far_r.at[phase, SECTIONS - k],
                    device_id=far_id(k),
                    device_id_type=MESH,
                )
            )
        return out

    def loc_copies(phase, src, dst):
        out = []
        for m in range(1, NEAR):
            out.append(
                pltpu.make_async_remote_copy(
                    src_ref=src(lax.rem(c + m, NEAR)),
                    dst_ref=dst,
                    send_sem=loc_s.at[phase, m],
                    recv_sem=loc_r.at[phase, NEAR - m],
                    device_id=loc_id(m),
                    device_id_type=MESH,
                )
            )
        return out

    def duo_copies(phase, src, dst):
        return [
            pltpu.make_async_remote_copy(
                src_ref=src,
                dst_ref=dst,
                send_sem=duo_s.at[phase],
                recv_sem=duo_r.at[phase],
                device_id=duo_id,
                device_id_type=MESH,
            )
        ]

    def start(copies):
        for copy in copies:
            copy.start()

    def wait(copies):
        for copy in copies:
            copy.wait()

    loads[4].wait()
    loads[5].wait()
    block = nrm.shape[2]
    squares = jnp.zeros((seqs, 1), F32)
    for i in range(ROW_BLOCKS):
        x = hid[:, i * block : (i + 1) * block].astype(F32)
        squares = squares + jnp.sum(x * x, -1, keepdims=True)
    factor = lax.rsqrt(squares * (1.0 / width) + 1e-05)
    for i in range(ROW_BLOCKS):
        x = hid[:, i * block : (i + 1) * block].astype(F32)
        y = (x * factor * gain[:, i * block : (i + 1) * block]).astype(BF16)
        nrm[i] = y.astype(F32)

    hear(1)
    tell(2)
    stream((3, 5), 2)

    per_section = ROW_BLOCKS // SECTIONS
    mine = [nrm[order[per_section * a + i]].astype(BF16) for i in range(per_section)]
    normed = jnp.concatenate(mine, -1)
    loads[0].wait()
    units = w.shape[0] // HEAD_DIM
    half = units // 2
    for u in range(units):
        y = nt_dot(normed, w_v[u * HEAD_DIM : (u + 1) * HEAD_DIM, :])
        for b in range(seqs):
            p_tx[2 * b + u // half, u % half : u % half + 1, :] = y[b : b + 1, :]
    own_rows = pl.ds(pl.multiple_of(a * cols, 8), cols)
    keep = pltpu.make_async_copy(w.at[own_rows, :], recv.at[a], load_sem.at[7])
    keep.start()

    hear(2)
    copies = far_copies(0, lambda b: p_tx.at[b], p_rx.at[a])
    start(copies)
    feed(next(feeds))
    p_rx[a] = p_tx[a]
    wait(copies)
    total = p_rx[0]
    for i in range(1, SECTIONS):
        total = total + p_rx[i]
    q_tx[0:half, :] = total.astype(BF16)
    q_all[s, c, a, 0:half, :] = total.astype(BF16)

    copies = far_copies(1, lambda b: q_tx, q_all.at[s, c, a])
    start(copies)
    feed(next(feeds))
    wait(copies)

    copies = loc_copies(0, lambda b: q_all.at[s, c], q_all.at[s, c])
    start(copies)
    feed(next(feeds))
    wait(copies)

    copies = duo_copies(0, q_all.at[s], q_all.at[s])
    start(copies)
    wait(copies)

    rotated = HEADS + KV_HEADS
    loads[6].wait()
    low = lax.broadcasted_iota(jnp.int32, (1, HEAD_DIM), 1) < 64

    def halves_of(row):
        turned = pltpu.roll(row, 64, 1)
        return jnp.where(low, row, turned), jnp.where(low, turned, row)

    for b in range(seqs):
        cos_hi, sin_hi = halves_of(table[pl.ds(lengths[b] // 64, 1), :])
        cos_lo, sin_lo = halves_of(table[pl.ds(HIGH_ROWS + lengths[b] % 64, 1), :])
        cosine = cos_hi * cos_lo - sin_hi * sin_lo
        sine = sin_hi * cos_lo + cos_hi * sin_lo
        sine = jnp.where(low, -sine, sine)
        for j in range(2 * SECTIONS):
            rank = j // 2
            rows[b, j * half : (j + 1) * half, :] = q_all[rank % 2, rank // 2, 2 * b + j % 2][
                :half
            ].astype(F32)
        x = rows[b, :rotated, :]
        x = x * cosine + pltpu.roll(x, 64, 1) * sine
        rows[b, :rotated, :] = x.astype(BF16).astype(F32)

    for copy in loads[1:3]:
        copy.wait()
    groups = HEADS // KV_HEADS
    inverse = 1.0 / math.sqrt(HEAD_DIM)
    pos_count = k_v.shape[1]
    first = (2 * t + s) * pos_count

    def one_sequence(b, carry):
        position = first + lax.broadcasted_iota(jnp.int32, (groups, pos_count), 1)
        usable = position < lengths[b]
        lane = lax.broadcasted_iota(jnp.int32, (groups, HEAD_DIM), 1)
        stats = []
        for k in range(KV_HEADS):
            lanes = slice(k * HEAD_DIM, (k + 1) * HEAD_DIM)
            q = rows[b, k * groups : (k + 1) * groups, :].astype(BF16)
            scores = nt_dot(q, k_v[b, :, lanes]) * inverse
            top = jnp.max(jnp.where(usable, scores, -1e30), -1, keepdims=True)
            weights = jnp.exp(jnp.where(usable, scores - top, -1e30))
            total = jnp.sum(weights, -1, keepdims=True)
            mix = jnp.dot(weights.astype(BF16), v_v[b, :, lanes], preferred_element_type=F32)
            stat = jnp.where((lane & 16) == 0, top, total)
            stats.append(jnp.where((lane >> 5) == b, stat, carry[k]))
            for g in range(groups):
                state[g % 2, g // 2, k, pl.ds(b, 1), :] = mix[g : g + 1, :]
        return tuple(stats)

    nothing = jnp.zeros((groups, HEAD_DIM), F32)
    stats = lax.fori_loop(0, seqs, one_sequence, (nothing,) * KV_HEADS)
    for k in range(KV_HEADS):
        for g in range(groups):
            state[g % 2, g // 2, k, seqs : seqs + 1, :] = stats[k][g : g + 1, :]

    def put(ref, part):
        mix, best, total = part
        low16 = (lax.broadcasted_iota(jnp.int32, best.shape, 1) & 16) == 0
        ref[0:seqs, :] = mix
        ref[seqs : seqs + 1, :] = jnp.where(low16, best, total)[0:1, :]

    copies = duo_copies(1, state.at[1 - s], a_rx1)
    start(copies)
    wait(copies)

    def merge_duo(i, carry):
        u, v = i // SECTIONS, i % SECTIONS
        put(a_tx.at[u, v], merged([state[s, u, v], a_rx1[u, v]], seqs))
        return carry

    lax.fori_loop(0, NEAR * SECTIONS, merge_duo, 0)

    copies = loc_copies(1, lambda m: a_tx.at[m], a_rx2.at[c])
    start(copies)
    feed(next(feeds))
    a_rx2[c] = a_tx[c]
    wait(copies)

    def merge_loc(v, carry):
        put(state.at[0, 0, v], merged([a_rx2[i, v] for i in range(NEAR)], seqs))
        return carry

    lax.fori_loop(0, SECTIONS, merge_loc, 0)

    copies = far_copies(2, lambda b: state.at[0, 0, b], a_rx3.at[a])
    start(copies)
    feed(next(feeds))
    a_rx3[a] = state[0, 0, a]
    wait(copies)
    mix, best, total = merged([a_rx3[i] for i in range(SECTIONS)], seqs)
    best, total = spread(best), spread(total)

    head = groups * a + 2 * c + s

    def head_rows(at):
        return jnp.concatenate([rows[b, pl.ds(at, 1), :] for b in range(seqs)], 0)

    own_score = jnp.sum(head_rows(head) * head_rows(HEADS + a), -1, keepdims=True) * inverse
    highest = jnp.maximum(best, own_score)
    old_scale = jnp.exp(best - highest)
    own_weight = jnp.exp(own_score - highest)
    numerator = mix * old_scale + own_weight * head_rows(rotated + a)
    denominator = total * old_scale + own_weight
    attended = (numerator / denominator).astype(BF16)

    loads[3].wait()
    wide = 512
    for i in range(width // wide):
        y = jnp.dot(attended, wo_v[:, i * wide : (i + 1) * wide], preferred_element_type=F32)
        for j in range(wide // 128):
            part[i * (wide // 128) + j] = y[:, j * 128 : (j + 1) * 128]

    half_blocks = part.shape[0] // 2
    own_half = pl.ds(s * half_blocks, half_blocks)
    copies = duo_copies(2, part.at[pl.ds((1 - s) * half_blocks, half_blocks)], o_rx1)
    start(copies)
    wait(copies)
    part[own_half] = part[own_half] + o_rx1[...]

    def quarter(m):
        return part.at[pl.ds(s * half_blocks + m * SECTIONS, SECTIONS)]

    copies = loc_copies(2, quarter, o_rx2.at[c])
    start(copies)
    feed(next(feeds))
    o_rx2[c] = part[pl.ds(s * half_blocks + c * SECTIONS, SECTIONS)]
    wait(copies)
    o_tx[...] = (o_rx2[0] + o_rx2[1]) + (o_rx2[2] + o_rx2[3])

    copies = far_copies(3, lambda b: o_tx.at[b], o_rx3.at[a])
    start(copies)
    feed(next(feeds))
    o_rx3[a] = o_tx[a]
    wait(copies)
    total = o_rx3[0]
    for i in range(1, SECTIONS):
        total = total + o_rx3[i]
    col = pl.multiple_of((s * half_blocks + c * SECTIONS + a) * 128, 128)
    g_all[s, c, a] = (hid[:, pl.ds(col, 128)].astype(F32) + total).astype(BF16)

    copies = far_copies(4, lambda b: g_all.at[s, c, a], g_all.at[s, c, a])
    start(copies)
    feed(next(feeds))
    wait(copies)

    copies = loc_copies(3, lambda m: g_all.at[s, c], g_all.at[s, c])
    start(copies)
    feed(next(feeds))
    wait(copies)

    copies = duo_copies(3, g_all.at[s], g_all.at[s])
    start(copies)
    while any(sent[k] < cols for k in everyone):
        stream(everyone, 1)
    wait(copies)
    give = pltpu.make_async_copy(g_all, g_out, load_sem.at[8])
    give.start()
    keep.wait()
    give.wait()
    for k in everyone:
        piece(k, 0, cols).wait()


def place_kernel(order, recv, g_in, mixed, new, out_sem):
    per_section = ROW_BLOCKS // SECTIONS
    block = recv.shape[2] // per_section
    writes = []
    for i in range(ROW_BLOCKS):
        at = pl.multiple_of(order[i] * block, 128)
        src = recv.at[i // per_section, :, pl.ds((i % per_section) * block, block)]
        copy = pltpu.make_async_copy(src, new.at[:, pl.ds(at, block)], out_sem.at[i])
        copy.start()
        writes.append(copy)
    blocks = g_in.shape[0] * g_in.shape[1] * g_in.shape[2]
    for j in range(blocks):
        mixed[:, j * 128 : (j + 1) * 128] = g_in[
            j // (NEAR * SECTIONS), (j // SECTIONS) % NEAR, j % SECTIONS
        ]
    for copy in writes:
        copy.wait()


def turn_table():
    half_dim = HEAD_DIM // 2
    freqs = 500000.0 ** (-np.arange(half_dim) * 2.0 / HEAD_DIM)
    steps = np.concatenate([64 * np.arange(HIGH_ROWS), np.arange(64)])
    angles = steps[:, None] * freqs[None, :]
    return np.concatenate([np.cos(angles), np.sin(angles)], -1).astype(np.float32)


def shards(hidden_in, norm_gain, wqkv_old, wo, key_cache, value_cache, lengths, section_order):
    seqs, width = hidden_in.shape
    _, _, rank_cols, rows_old = wqkv_old.shape
    cols = rank_cols // SECTIONS
    block = width // ROW_BLOCKS
    pos_count = key_cache.shape[1]

    vmem = pl.BlockSpec(memory_space=pltpu.VMEM)
    smem = pl.BlockSpec(memory_space=pltpu.SMEM)
    hbm = pl.BlockSpec(memory_space=pl.ANY)
    dma = pltpu.SemaphoreType.DMA
    tile, five = (8, 128), (seqs + 1, 128)
    recv, g_out = pl.pallas_call(
        main_kernel,
        name="stream_and_decode",
        out_shape=(
            pltpu.VMEM((SECTIONS, cols, rows_old), BF16),
            jax.ShapeDtypeStruct((2, NEAR, SECTIONS, seqs, 128), BF16),
        ),
        in_specs=[hbm, hbm, hbm, smem, smem, hbm, hbm, hbm, hbm],
        out_specs=(vmem, hbm),
        scratch_shapes=[
            pltpu.VMEM((seqs, width), BF16),
            pltpu.VMEM((1, width), F32),
            pltpu.VMEM((HIGH_ROWS + 64, HEAD_DIM), F32),
            pltpu.VMEM((rank_cols, rows_old), BF16),
            pltpu.VMEM(wo.shape, BF16),
            pltpu.VMEM(key_cache.shape, BF16),
            pltpu.VMEM(value_cache.shape, BF16),
            pltpu.VMEM((ROW_BLOCKS, seqs, block), F32),
            pltpu.VMEM((SECTIONS, *five), F32),
            pltpu.VMEM((SECTIONS, *five), F32),
            pltpu.VMEM(tile, BF16),
            pltpu.VMEM((2, NEAR, SECTIONS, *tile), BF16),
            pltpu.VMEM((seqs, HEADS + 2 * KV_HEADS, HEAD_DIM), F32),
            pltpu.VMEM((2, NEAR, SECTIONS, *five), F32),
            pltpu.VMEM((NEAR, SECTIONS, *five), F32),
            pltpu.VMEM((NEAR, SECTIONS, *five), F32),
            pltpu.VMEM((NEAR, SECTIONS, *five), F32),
            pltpu.VMEM((SECTIONS, *five), F32),
            pltpu.VMEM((width // 128, seqs, 128), F32),
            pltpu.VMEM((width // 256, seqs, 128), F32),
            pltpu.VMEM((NEAR, SECTIONS, seqs, 128), F32),
            pltpu.VMEM((SECTIONS, seqs, 128), F32),
            pltpu.VMEM((SECTIONS, seqs, 128), F32),
            pltpu.VMEM((2, NEAR, SECTIONS, seqs, 128), BF16),
            dma((9,)),
            dma((SECTIONS,)),
            dma((SECTIONS,)),
            dma((5, SECTIONS)),
            dma((5, SECTIONS)),
            dma((4, NEAR)),
            dma((4, NEAR)),
            dma((4,)),
            dma((4,)),
            pltpu.SemaphoreType.REGULAR((3,)),
            pltpu.SemaphoreType.REGULAR((3,)),
        ],
        compiler_params=pltpu.CompilerParams(collective_id=0, has_side_effects=True),
    )(
        hidden_in,
        norm_gain.reshape(1, width),
        jnp.asarray(turn_table()),
        lengths,
        section_order,
        wqkv_old.reshape(rank_cols, rows_old),
        wo,
        key_cache,
        value_cache,
    )

    mixed_out, new_weight = pl.pallas_call(
        place_kernel,
        name="place",
        out_shape=(
            jax.ShapeDtypeStruct((seqs, width), BF16),
            jax.ShapeDtypeStruct((cols, width), BF16),
        ),
        in_specs=[smem, vmem, vmem],
        out_specs=(vmem, hbm),
        scratch_shapes=[dma((ROW_BLOCKS,))],
    )(section_order, pltpu.with_memory_space_constraint(recv, pltpu.VMEM), g_out)
    return mixed_out, new_weight[None, None]


def solution(mesh):
    placed = (
        P("replica", None),
        P("replica"),
        P(("replica", "tp"), "sub", None, None),
        P(("replica", "tp", "sub"), None),
        P("replica", ("tp", "sub"), None),
        P("replica", ("tp", "sub"), None),
        P("replica"),
        P("replica"),
    )
    return jax.shard_map(
        shards,
        mesh=mesh,
        in_specs=placed,
        out_specs=(P("replica", None), P(("replica", "tp"), "sub", None, None)),
        check_vma=False,
    )
```

```python
import functools
import math

import jax
import jax.numpy as jnp
import numpy as np
from jax import lax
from jax.experimental import pallas as pl
from jax.experimental.pallas import tpu as pltpu
from jax.sharding import PartitionSpec as P

HEADS = 64
KV_HEADS = 8
HEAD_DIM = 128
ROW_BLOCKS = 16
NEAR = 4
SECTIONS = 8
FEEDS = (0, 0, 0, 1, 1, 1, 1, 1)
HIGH_ROWS = 72
STEP_ROWS = 16

FIRST = (4, 2, 1, 0)
MESH = pl.DeviceIdType.MESH
F32 = jnp.float32
BF16 = jnp.bfloat16


def nt_dot(x, y):
    return lax.dot_general(x, y, (((1,), (1,)), ((), ())), preferred_element_type=F32)


def spread(x):
    lane = lax.broadcasted_iota(jnp.int32, x.shape, 1)
    row = lax.broadcasted_iota(jnp.int32, x.shape, 0)
    return jnp.max(jnp.where((lane >> 5) == row, x, -3e38), -1, keepdims=True)


def merged(tiles, seqs):
    tops, totals = [], []
    low = (lax.broadcasted_iota(jnp.int32, (seqs, 128), 1) & 16) == 0
    for tile in tiles:
        stat = jnp.broadcast_to(tile[seqs : seqs + 1, :], (seqs, 128))
        tops.append(jnp.where(low, stat, pltpu.roll(stat, 16, 1)))
        totals.append(jnp.where(low, pltpu.roll(stat, 112, 1), stat))
    best = functools.reduce(jnp.maximum, tops)
    mix, total = None, None
    for tile, top, s in zip(tiles, tops, totals):
        f = jnp.exp(top - best)
        m = tile[0:seqs, :] * spread(f)
        mix = m if mix is None else mix + m
        total = s * f if total is None else total + s * f
    return mix, best, total


def main_kernel(
    hid_in, gain_in, table_in, lengths, order, w, wo, kc, vc,
    recv, g_out,
    hid, gain, table, w_v, wo_v, k_v, v_v, nrm, p_tx, p_rx, q_tx, q_all, rows, state, a_rx1, a_rx2,
    a_tx, a_rx3, heads, part, o_rx1, o_rx2, o_tx, o_rx3, g_all,
    load_sem, big_s, big_r, far_s, far_r, loc_s, loc_r, duo_s, duo_r, known_lo, known_hi,
):
    count = lax.axis_size("tp")
    t = lax.axis_index("tp")
    s = lax.axis_index("sub")
    a = t // NEAR
    c = t % NEAR
    seqs, width = hid_in.shape
    cols = recv.shape[1]
    leads, helps = s == 1, s == 0

    def far_id(k):
        return {"tp": lax.rem(t + NEAR * k, count)}

    def loc_id(d):
        return {"tp": lax.rem(t + d + count, count)}

    duo_id = {"sub": 1 - s}

    barrier = pltpu.get_barrier_semaphore()
    greeted = [loc_id(d) for d in (1, -1, 2, -2, NEAR, -NEAR)] + [duo_id]
    for target in greeted:
        pl.semaphore_signal(barrier, inc=1, device_id=target, device_id_type=MESH)

    loads = [
        pltpu.make_async_copy(src, dst, load_sem.at[i])
        for i, (src, dst) in enumerate(
            (
                (w, w_v),
                (kc, k_v),
                (vc, v_v),
                (wo, wo_v),
                (hid_in, hid),
                (gain_in, gain),
                (table_in, table),
            )
        )
    ]
    for i in (4, 5, 0):
        loads[i].start()
    pl.semaphore_wait(barrier, len(greeted))

    def piece(k, row, height):
        b = lax.rem(a + k, SECTIONS)
        first = pl.multiple_of(b * cols + row, 8)
        return pltpu.make_async_remote_copy(
            src_ref=w.at[pl.ds(first, height), :],
            dst_ref=recv.at[a, pl.ds(row, height), :],
            send_sem=big_s.at[k],
            recv_sem=big_r.at[SECTIONS - k],
            device_id=far_id(k),
            device_id_type=MESH,
        )

    sent = {}

    def stream(core, ks, n):
        ks = [k for k in ks if sent.get((core, k), 0) < cols]
        n = min([n] + [(cols - sent.get((core, k), 0)) // STEP_ROWS for k in ks])
        if not ks or n == 0:
            return
        starts = {k: sent.get((core, k), 0) for k in ks}

        def body(i, carry):
            for k in ks:
                piece(k, pl.multiple_of(starts[k] + i * STEP_ROWS, 8), STEP_ROWS).start()
            return carry

        @pl.when(s == core)
        def _():
            lax.fori_loop(0, n, body, 0)

        for k in ks:
            sent[core, k] = starts[k] + n * STEP_ROWS

    everyone = (4, 3, 5, 2, 6, 1, 7)
    feeds = iter(FEEDS)

    def stream_rest(core):
        while any(sent.get((core, k), 0) < cols for k in everyone):
            stream(core, everyone, cols // STEP_ROWS)

    def tell(stage):
        pl.semaphore_signal(known_lo.at[stage], inc=1, device_id=far_id(1), device_id_type=MESH)
        pl.semaphore_signal(
            known_hi.at[stage], inc=1, device_id=far_id(SECTIONS - 1), device_id_type=MESH
        )

    def hear(stage):
        pl.semaphore_wait(known_lo.at[stage], 1)
        pl.semaphore_wait(known_hi.at[stage], 1)

    tell(0)
    stream(0, (1, 7), FIRST[0])
    stream(1, (1, 7), FIRST[3])
    for i in (6, 1, 2, 3):
        loads[i].start()
    hear(0)
    tell(1)
    stream(0, (2, 6), FIRST[1])

    def remote(src, dst, send_sem, recv_sem, target):
        return pltpu.make_async_remote_copy(
            src_ref=src,
            dst_ref=dst,
            send_sem=send_sem,
            recv_sem=recv_sem,
            device_id=target,
            device_id_type=MESH,
        )

    def far_copies(phase, src, dst):
        return [
            remote(
                src(lax.rem(a + k, SECTIONS)),
                dst,
                far_s.at[phase, k],
                far_r.at[phase, SECTIONS - k],
                far_id(k),
            )
            for k in (4, 3, 5, 2, 6, 1, 7)
        ]

    def loc_copies(phase, src, dst):
        out = []
        for i, (d, h) in enumerate(((1, None), (-1, None), (2, 0), (-2, 1))):
            place = lax.rem(c + d + NEAR, NEAR)
            sems = loc_s.at[phase, i], loc_r.at[phase, i]
            out.append(remote(src(place, h), dst(min(i, 2), h), *sems, loc_id(d)))
        return out

    def part_of(ref, at, size, h):
        if h is None:
            return ref.at[pl.ds(at, size)]
        return ref.at[pl.ds(at + h * (size // 2), size // 2)]

    def duo_copy(phase, src, dst):
        return remote(src, dst, duo_s.at[phase], duo_r.at[phase], duo_id)

    def start(copies):
        for copy in copies:
            copy.start()

    def wait(copies):
        for copy in copies:
            copy.wait()

    loads[4].wait()
    loads[5].wait()
    block = nrm.shape[2]
    squares = jnp.zeros((seqs, 1), F32)
    for i in range(ROW_BLOCKS):
        x = hid[:, i * block : (i + 1) * block].astype(F32)
        squares = squares + jnp.sum(x * x, -1, keepdims=True)
    factor = lax.rsqrt(squares * (1.0 / width) + 1e-05)
    for i in range(ROW_BLOCKS):
        x = hid[:, i * block : (i + 1) * block].astype(F32)
        y = (x * factor * gain[:, i * block : (i + 1) * block]).astype(BF16)
        nrm[i] = y.astype(F32)

    hear(1)
    tell(2)
    stream(0, (3, 5), FIRST[2])

    per_section = ROW_BLOCKS // SECTIONS
    mine = [nrm[order[per_section * a + i]].astype(BF16) for i in range(per_section)]
    normed = jnp.concatenate(mine, -1)
    loads[0].wait()
    units = w.shape[0] // HEAD_DIM
    half = units // 2
    for u in range(units):
        y = nt_dot(normed, w_v[u * HEAD_DIM : (u + 1) * HEAD_DIM, :])
        for b in range(seqs):
            p_tx[2 * b + u // half, s, u % half : u % half + 1, :] = y[b : b + 1, :]
    own_rows = pl.ds(pl.multiple_of(a * cols, 8), cols)
    keep = pltpu.make_async_copy(w.at[own_rows, :], recv.at[a], load_sem.at[7])
    keep.start()

    hear(2)
    def own_q(_, h):
        return part_of(q_all.at[c], 0, SECTIONS, h)

    def own_g(_, h):
        return part_of(g_all.at[c], 0, SECTIONS, h)

    give_p = duo_copy(0, p_tx.at[:, 0], p_tx.at[:, 0])
    give_q = duo_copy(1, q_all, q_all)

    @pl.when(helps)
    def _():
        give_p.start()

    stream_rest(0)

    @pl.when(helps)
    def _():
        give_p.wait_send()
        give_q.wait_recv()

    @pl.when(leads)
    def _():
        give_p.wait_recv()
        copies = far_copies(0, lambda b: p_tx.at[b], p_rx.at[a])
        start(copies)
        stream(1, everyone, next(feeds))
        p_rx[a] = p_tx[a]
        wait(copies)
        total = p_rx[0]
        for i in range(1, SECTIONS):
            total = total + p_rx[i]
        q_tx[:, 0:half, :] = total.astype(BF16)
        q_all[c, a, :, 0:half, :] = total.astype(BF16)

        copies = far_copies(1, lambda b: q_tx, q_all.at[c, a])
        start(copies)
        stream(1, everyone, next(feeds))
        wait(copies)

        copies = loc_copies(0, own_q, own_q)
        start(copies)
        stream(1, everyone, next(feeds))
        wait(copies)
        give_q.start()
        give_q.wait_send()

    rotated = HEADS + KV_HEADS
    loads[6].wait()
    low = lax.broadcasted_iota(jnp.int32, (1, HEAD_DIM), 1) < 64

    def halves_of(row):
        turned = pltpu.roll(row, 64, 1)
        return jnp.where(low, row, turned), jnp.where(low, turned, row)

    for b in range(seqs):
        cos_hi, sin_hi = halves_of(table[pl.ds(lengths[b] // 64, 1), :])
        cos_lo, sin_lo = halves_of(table[pl.ds(HIGH_ROWS + lengths[b] % 64, 1), :])
        cosine = cos_hi * cos_lo - sin_hi * sin_lo
        sine = sin_hi * cos_lo + cos_hi * sin_lo
        sine = jnp.where(low, -sine, sine)
        for j in range(2 * SECTIONS):
            rank = j // 2
            rows[b, j * half : (j + 1) * half, :] = q_all[rank // 2, 2 * b + j % 2, rank % 2][
                :half
            ].astype(F32)
        x = rows[b, :rotated, :]
        x = x * cosine + pltpu.roll(x, 64, 1) * sine
        rows[b, :rotated, :] = x.astype(BF16).astype(F32)

    for copy in loads[1:3]:
        copy.wait()
    groups = HEADS // KV_HEADS
    inverse = 1.0 / math.sqrt(HEAD_DIM)
    pos_count = k_v.shape[1]
    first = (2 * t + s) * pos_count

    def one_sequence(b, carry):
        position = first + lax.broadcasted_iota(jnp.int32, (groups, pos_count), 1)
        usable = position < lengths[b]
        lane = lax.broadcasted_iota(jnp.int32, (groups, HEAD_DIM), 1)
        stats = []
        for k in range(KV_HEADS):
            lanes = slice(k * HEAD_DIM, (k + 1) * HEAD_DIM)
            q = rows[b, k * groups : (k + 1) * groups, :].astype(BF16)
            scores = nt_dot(q, k_v[b, :, lanes]) * inverse
            top = jnp.max(jnp.where(usable, scores, -1e30), -1, keepdims=True)
            weights = jnp.exp(jnp.where(usable, scores - top, -1e30))
            total = jnp.sum(weights, -1, keepdims=True)
            mix = jnp.dot(weights.astype(BF16), v_v[b, :, lanes], preferred_element_type=F32)
            stat = jnp.where((lane & 16) == 0, top, total)
            stats.append(jnp.where((lane >> 5) == b, stat, carry[k]))
            for g in range(groups):
                state[g // 2, k, g % 2, pl.ds(b, 1), :] = mix[g : g + 1, :]
        return tuple(stats)

    nothing = jnp.zeros((groups, HEAD_DIM), F32)
    stats = lax.fori_loop(0, seqs, one_sequence, (nothing,) * KV_HEADS)
    for k in range(KV_HEADS):
        for g in range(groups):
            state[g // 2, k, g % 2, seqs : seqs + 1, :] = stats[k][g : g + 1, :]

    def put(ref, part):
        mix, best, total = part
        low16 = (lax.broadcasted_iota(jnp.int32, best.shape, 1) & 16) == 0
        ref[0:seqs, :] = mix
        ref[seqs : seqs + 1, :] = jnp.where(low16, best, total)[0:1, :]

    give_state = duo_copy(2, state, a_rx1)
    give_head = duo_copy(3, heads.at[0], heads.at[0])

    @pl.when(helps)
    def _():
        give_state.start()
        give_state.wait_send()
        give_head.wait_recv()

    @pl.when(leads)
    def _():
        give_state.wait_recv()

        def merge_duo(i, carry):
            u, v = i // SECTIONS, i % SECTIONS
            for e in range(2):
                put(a_tx.at[u, v, e], merged([state[u, v, e], a_rx1[u, v, e]], seqs))
            return carry

        lax.fori_loop(0, NEAR * SECTIONS, merge_duo, 0, unroll=2)

        copies = loc_copies(
            1,
            lambda place, h: part_of(a_tx.at[place], 0, SECTIONS, h),
            lambda i, h: part_of(a_rx2.at[i], 0, SECTIONS, h),
        )
        start(copies)
        stream(1, everyone, next(feeds))
        a_rx2[3] = a_tx[c]
        wait(copies)

        def merge_loc(v, carry):
            for e in range(2):
                put(state.at[0, v, e], merged([a_rx2[i, v, e] for i in range(NEAR)], seqs))
            return carry

        lax.fori_loop(0, SECTIONS, merge_loc, 0)

        copies = far_copies(2, lambda b: state.at[0, b], a_rx3.at[a])
        start(copies)
        stream(1, everyone, next(feeds))
        a_rx3[a] = state[0, a]
        wait(copies)

        def head_rows(at):
            return jnp.concatenate([rows[b, pl.ds(at, 1), :] for b in range(seqs)], 0)

        for e in range(2):
            mix, best, total = merged([a_rx3[i, e] for i in range(SECTIONS)], seqs)
            best, total = spread(best), spread(total)
            head = groups * a + 2 * c + e
            products = head_rows(head) * head_rows(HEADS + a)
            own_score = jnp.sum(products, -1, keepdims=True) * inverse
            highest = jnp.maximum(best, own_score)
            old_scale = jnp.exp(best - highest)
            own_weight = jnp.exp(own_score - highest)
            numerator = mix * old_scale + own_weight * head_rows(rotated + a)
            denominator = total * old_scale + own_weight
            heads[e] = (numerator / denominator).astype(BF16).astype(F32)
        give_head.start()
        give_head.wait_send()

    loads[3].wait()
    attended = heads[s].astype(BF16)
    wide = 512
    for i in range(width // wide):
        y = jnp.dot(attended, wo_v[:, i * wide : (i + 1) * wide], preferred_element_type=F32)
        for j in range(wide // 128):
            part[i * (wide // 128) + j] = y[:, j * 128 : (j + 1) * 128]

    give_part = duo_copy(4, part, o_rx1)
    give_out = duo_copy(5, g_all, g_all)
    quarter = part.shape[0] // NEAR

    @pl.when(helps)
    def _():
        give_part.start()
        give_part.wait_send()
        give_out.wait_recv()

    @pl.when(leads)
    def _():
        give_part.wait_recv()
        part[...] = part[...] + o_rx1[...]
        copies = loc_copies(
            2,
            lambda place, h: part_of(part, place * quarter, quarter, h),
            lambda i, h: part_of(o_rx2.at[i], 0, quarter, h),
        )
        start(copies)
        stream(1, everyone, next(feeds))
        o_rx2[3] = part[pl.ds(c * quarter, quarter)]
        wait(copies)
        o_tx[...] = (o_rx2[0] + o_rx2[1]) + (o_rx2[2] + o_rx2[3])

        copies = far_copies(3, lambda b: o_tx.at[pl.ds(2 * b, 2)], o_rx3.at[a])
        start(copies)
        stream(1, everyone, next(feeds))
        o_rx3[a] = o_tx[pl.ds(2 * a, 2)]
        wait(copies)
        total = o_rx3[0]
        for i in range(1, SECTIONS):
            total = total + o_rx3[i]
        for e in range(2):
            col = pl.multiple_of((c * quarter + 2 * a + e) * 128, 128)
            g_all[c, a, e] = (hid[:, pl.ds(col, 128)].astype(F32) + total[e]).astype(BF16)

        copies = far_copies(4, lambda b: g_all.at[c, a], g_all.at[c, a])
        start(copies)
        stream(1, everyone, next(feeds))
        wait(copies)

        copies = loc_copies(3, own_g, own_g)
        start(copies)

    stream_rest(1)

    @pl.when(leads)
    def _():
        wait(loc_copies(3, own_g, own_g))
        give_out.start()
        give_out.wait_send()

    give = pltpu.make_async_copy(g_all, g_out, load_sem.at[8])
    give.start()
    keep.wait()
    give.wait()
    for k in everyone:
        piece(k, 0, cols).wait()


def place_kernel(order, recv, g_in, mixed, new, out_sem):
    per_section = ROW_BLOCKS // SECTIONS
    block = recv.shape[2] // per_section
    writes = []
    for i in range(ROW_BLOCKS):
        at = pl.multiple_of(order[i] * block, 128)
        src = recv.at[i // per_section, :, pl.ds((i % per_section) * block, block)]
        copy = pltpu.make_async_copy(src, new.at[:, pl.ds(at, block)], out_sem.at[i])
        copy.start()
        writes.append(copy)
    blocks = g_in.shape[0] * g_in.shape[1] * g_in.shape[2]
    for j in range(blocks):
        mixed[:, j * 128 : (j + 1) * 128] = g_in[
            j // (2 * SECTIONS), (j // 2) % SECTIONS, j % 2
        ]
    for copy in writes:
        copy.wait()


def turn_table():
    half_dim = HEAD_DIM // 2
    freqs = 500000.0 ** (-np.arange(half_dim) * 2.0 / HEAD_DIM)
    steps = np.concatenate([64 * np.arange(HIGH_ROWS), np.arange(64)])
    angles = steps[:, None] * freqs[None, :]
    return np.concatenate([np.cos(angles), np.sin(angles)], -1).astype(np.float32)


def shards(hidden_in, norm_gain, wqkv_old, wo, key_cache, value_cache, lengths, section_order):
    seqs, width = hidden_in.shape
    _, _, rank_cols, rows_old = wqkv_old.shape
    cols = rank_cols // SECTIONS
    block = width // ROW_BLOCKS
    pos_count = key_cache.shape[1]

    vmem = pl.BlockSpec(memory_space=pltpu.VMEM)
    smem = pl.BlockSpec(memory_space=pltpu.SMEM)
    hbm = pl.BlockSpec(memory_space=pl.ANY)
    dma = pltpu.SemaphoreType.DMA
    tile, five = (8, 128), (seqs + 1, 128)
    recv, g_out = pl.pallas_call(
        main_kernel,
        name="stream_and_decode",
        out_shape=(
            pltpu.VMEM((SECTIONS, cols, rows_old), BF16),
            jax.ShapeDtypeStruct((NEAR, SECTIONS, 2, seqs, 128), BF16),
        ),
        in_specs=[hbm, hbm, hbm, smem, smem, hbm, hbm, hbm, hbm],
        out_specs=(vmem, hbm),
        scratch_shapes=[
            pltpu.VMEM((seqs, width), BF16),
            pltpu.VMEM((1, width), F32),
            pltpu.VMEM((HIGH_ROWS + 64, HEAD_DIM), F32),
            pltpu.VMEM((rank_cols, rows_old), BF16),
            pltpu.VMEM(wo.shape, BF16),
            pltpu.VMEM(key_cache.shape, BF16),
            pltpu.VMEM(value_cache.shape, BF16),
            pltpu.VMEM((ROW_BLOCKS, seqs, block), F32),
            pltpu.VMEM((SECTIONS, 2, *five), F32),
            pltpu.VMEM((SECTIONS, 2, *five), F32),
            pltpu.VMEM((2, *tile), BF16),
            pltpu.VMEM((NEAR, SECTIONS, 2, *tile), BF16),
            pltpu.VMEM((seqs, HEADS + 2 * KV_HEADS, HEAD_DIM), F32),
            pltpu.VMEM((NEAR, SECTIONS, 2, *five), F32),
            pltpu.VMEM((NEAR, SECTIONS, 2, *five), F32),
            pltpu.VMEM((NEAR, SECTIONS, 2, *five), F32),
            pltpu.VMEM((NEAR, SECTIONS, 2, *five), F32),
            pltpu.VMEM((SECTIONS, 2, *five), F32),
            pltpu.VMEM((2, seqs, HEAD_DIM), F32),
            pltpu.VMEM((width // 128, seqs, 128), F32),
            pltpu.VMEM((width // 128, seqs, 128), F32),
            pltpu.VMEM((NEAR, width // 512, seqs, 128), F32),
            pltpu.VMEM((width // 512, seqs, 128), F32),
            pltpu.VMEM((SECTIONS, 2, seqs, 128), F32),
            pltpu.VMEM((NEAR, SECTIONS, 2, seqs, 128), BF16),
            dma((9,)),
            dma((SECTIONS,)),
            dma((SECTIONS,)),
            dma((5, SECTIONS)),
            dma((5, SECTIONS)),
            dma((4, NEAR)),
            dma((4, NEAR)),
            dma((6,)),
            dma((6,)),
            pltpu.SemaphoreType.REGULAR((3,)),
            pltpu.SemaphoreType.REGULAR((3,)),
        ],
        compiler_params=pltpu.CompilerParams(collective_id=0, has_side_effects=True),
    )(
        hidden_in,
        norm_gain.reshape(1, width),
        jnp.asarray(turn_table()),
        lengths,
        section_order,
        wqkv_old.reshape(rank_cols, rows_old),
        wo,
        key_cache,
        value_cache,
    )

    mixed_out, new_weight = pl.pallas_call(
        place_kernel,
        name="place",
        out_shape=(
            jax.ShapeDtypeStruct((seqs, width), BF16),
            jax.ShapeDtypeStruct((cols, width), BF16),
        ),
        in_specs=[smem, vmem, vmem],
        out_specs=(vmem, hbm),
        scratch_shapes=[dma((ROW_BLOCKS,))],
    )(section_order, pltpu.with_memory_space_constraint(recv, pltpu.VMEM), g_out)
    return mixed_out, new_weight[None, None]


def solution(mesh):
    placed = (
        P("replica", None),
        P("replica"),
        P(("replica", "tp"), "sub", None, None),
        P(("replica", "tp", "sub"), None),
        P("replica", ("tp", "sub"), None),
        P("replica", ("tp", "sub"), None),
        P("replica"),
        P("replica"),
    )
    return jax.shard_map(
        shards,
        mesh=mesh,
        in_specs=placed,
        out_specs=(P("replica", None), P(("replica", "tp"), "sub", None, None)),
        check_vma=False,
    )
```

```python
import functools
import math

import jax
import jax.numpy as jnp
import numpy as np
from jax import lax
from jax.experimental import pallas as pl
from jax.experimental.pallas import tpu as pltpu
from jax.sharding import PartitionSpec as P

HEADS = 64
KV_HEADS = 8
HEAD_DIM = 128
ROW_BLOCKS = 16
NEAR = 4
SECTIONS = 8
FEEDS = (0, 0, 0, 1, 1, 1, 1, 1)
HIGH_ROWS = 72
STEP_ROWS = 16

FIRST = (4, 2, 1, 0)
MESH = pl.DeviceIdType.MESH
F32 = jnp.float32
BF16 = jnp.bfloat16


def nt_dot(x, y):
    return lax.dot_general(x, y, (((1,), (1,)), ((), ())), preferred_element_type=F32)


def spread(x):
    lane = lax.broadcasted_iota(jnp.int32, x.shape, 1)
    row = lax.broadcasted_iota(jnp.int32, x.shape, 0)
    return jnp.max(jnp.where((lane >> 5) == row, x, -3e38), -1, keepdims=True)


def merged(tiles, seqs):
    tops, totals = [], []
    low = (lax.broadcasted_iota(jnp.int32, (seqs, 128), 1) & 16) == 0
    for tile in tiles:
        stat = jnp.broadcast_to(tile[seqs : seqs + 1, :], (seqs, 128))
        tops.append(jnp.where(low, stat, pltpu.roll(stat, 16, 1)))
        totals.append(jnp.where(low, pltpu.roll(stat, 112, 1), stat))
    best = functools.reduce(jnp.maximum, tops)
    mix, total = None, None
    for tile, top, s in zip(tiles, tops, totals):
        f = jnp.exp(top - best)
        m = tile[0:seqs, :] * spread(f)
        mix = m if mix is None else mix + m
        total = s * f if total is None else total + s * f
    return mix, best, total


def main_kernel(
    hid_in, gain_in, table_in, lengths, order, w, wo, kc, vc,
    recv, g_all,
    hid, gain, table, w_v, wo_v, k_v, v_v, nrm, p_tx, p_rx, q_tx, q_all, rows, state, a_rx1, a_rx2,
    a_tx, a_rx3, heads, part, o_rx1, o_rx2, o_tx, o_rx3,
    load_sem, big_s, big_r, far_s, far_r, loc_s, loc_r, duo_s, duo_r, known_lo, known_hi,
):
    count = lax.axis_size("tp")
    t = lax.axis_index("tp")
    s = lax.axis_index("sub")
    a = t // NEAR
    c = t % NEAR
    seqs, width = hid_in.shape
    cols = recv.shape[1]
    leads, helps = s == 1, s == 0

    def far_id(k):
        return {"tp": lax.rem(t + NEAR * k, count)}

    def loc_id(d):
        return {"tp": lax.rem(t + d + count, count)}

    duo_id = {"sub": 1 - s}

    barrier = pltpu.get_barrier_semaphore()
    greeted = [loc_id(d) for d in (1, -1, 2, -2, NEAR, -NEAR)] + [duo_id]
    for target in greeted:
        pl.semaphore_signal(barrier, inc=1, device_id=target, device_id_type=MESH)

    loads = [
        pltpu.make_async_copy(src, dst, load_sem.at[i])
        for i, (src, dst) in enumerate(
            (
                (w, w_v),
                (kc, k_v),
                (vc, v_v),
                (wo, wo_v),
                (hid_in, hid),
                (gain_in, gain),
                (table_in, table),
            )
        )
    ]
    for i in (4, 5, 0):
        loads[i].start()
    pl.semaphore_wait(barrier, len(greeted))

    def piece(k, row, height):
        b = lax.rem(a + k, SECTIONS)
        first = pl.multiple_of(b * cols + row, 8)
        return pltpu.make_async_remote_copy(
            src_ref=w.at[pl.ds(first, height), :],
            dst_ref=recv.at[a, pl.ds(row, height), :],
            send_sem=big_s.at[k],
            recv_sem=big_r.at[SECTIONS - k],
            device_id=far_id(k),
            device_id_type=MESH,
        )

    sent = {}

    def stream(core, ks, n):
        ks = [k for k in ks if sent.get((core, k), 0) < cols]
        n = min([n] + [(cols - sent.get((core, k), 0)) // STEP_ROWS for k in ks])
        if not ks or n == 0:
            return
        starts = {k: sent.get((core, k), 0) for k in ks}

        def body(i, carry):
            for k in ks:
                piece(k, pl.multiple_of(starts[k] + i * STEP_ROWS, 8), STEP_ROWS).start()
            return carry

        @pl.when(s == core)
        def _():
            lax.fori_loop(0, n, body, 0)

        for k in ks:
            sent[core, k] = starts[k] + n * STEP_ROWS

    everyone = (4, 3, 5, 2, 6, 1, 7)
    feeds = iter(FEEDS)

    def stream_rest(core):
        while any(sent.get((core, k), 0) < cols for k in everyone):
            stream(core, everyone, cols // STEP_ROWS)

    def tell(stage):
        pl.semaphore_signal(known_lo.at[stage], inc=1, device_id=far_id(1), device_id_type=MESH)
        pl.semaphore_signal(
            known_hi.at[stage], inc=1, device_id=far_id(SECTIONS - 1), device_id_type=MESH
        )

    def hear(stage):
        pl.semaphore_wait(known_lo.at[stage], 1)
        pl.semaphore_wait(known_hi.at[stage], 1)

    tell(0)
    stream(0, (1, 7), FIRST[0])
    stream(1, (1, 7), FIRST[3])
    for i in (6, 1, 2, 3):
        loads[i].start()
    hear(0)
    tell(1)
    stream(0, (2, 6), FIRST[1])

    def remote(src, dst, send_sem, recv_sem, target):
        return pltpu.make_async_remote_copy(
            src_ref=src,
            dst_ref=dst,
            send_sem=send_sem,
            recv_sem=recv_sem,
            device_id=target,
            device_id_type=MESH,
        )

    def far_copies(phase, src, dst):
        return [
            remote(
                src(lax.rem(a + k, SECTIONS)),
                dst,
                far_s.at[phase, k],
                far_r.at[phase, SECTIONS - k],
                far_id(k),
            )
            for k in (4, 3, 5, 2, 6, 1, 7)
        ]

    def loc_copies(phase, src, dst):
        out = []
        for i, (d, h) in enumerate(((1, None), (-1, None), (2, 0), (-2, 1))):
            place = lax.rem(c + d + NEAR, NEAR)
            sems = loc_s.at[phase, i], loc_r.at[phase, i]
            out.append(remote(src(place, h), dst(min(i, 2), h), *sems, loc_id(d)))
        return out

    def part_of(ref, at, size, h):
        if h is None:
            return ref.at[pl.ds(at, size)]
        return ref.at[pl.ds(at + h * (size // 2), size // 2)]

    def duo_copy(phase, src, dst):
        return remote(src, dst, duo_s.at[phase], duo_r.at[phase], duo_id)

    def start(copies):
        for copy in copies:
            copy.start()

    def wait(copies):
        for copy in copies:
            copy.wait()

    loads[4].wait()
    loads[5].wait()
    block = nrm.shape[2]
    squares = jnp.zeros((seqs, 1), F32)
    for i in range(ROW_BLOCKS):
        x = hid[:, i * block : (i + 1) * block].astype(F32)
        squares = squares + jnp.sum(x * x, -1, keepdims=True)
    factor = lax.rsqrt(squares * (1.0 / width) + 1e-05)
    for i in range(ROW_BLOCKS):
        x = hid[:, i * block : (i + 1) * block].astype(F32)
        y = (x * factor * gain[:, i * block : (i + 1) * block]).astype(BF16)
        nrm[i] = y.astype(F32)

    hear(1)
    tell(2)
    stream(0, (3, 5), FIRST[2])

    per_section = ROW_BLOCKS // SECTIONS
    mine = [nrm[order[per_section * a + i]].astype(BF16) for i in range(per_section)]
    normed = jnp.concatenate(mine, -1)
    loads[0].wait()
    units = w.shape[0] // HEAD_DIM
    half = units // 2
    for u in range(units):
        y = nt_dot(normed, w_v[u * HEAD_DIM : (u + 1) * HEAD_DIM, :])
        for b in range(seqs):
            p_tx[2 * b + u // half, s, u % half : u % half + 1, :] = y[b : b + 1, :]
    own_rows = pl.ds(pl.multiple_of(a * cols, 8), cols)
    keep = pltpu.make_async_copy(w.at[own_rows, :], recv.at[a], load_sem.at[7])
    keep.start()

    hear(2)
    def own_q(_, h):
        return part_of(q_all.at[c], 0, SECTIONS, h)

    def own_g(_, h):
        return part_of(g_all.at[c], 0, SECTIONS, h)

    give_p = duo_copy(0, p_tx.at[:, 0], p_tx.at[:, 0])
    give_q = duo_copy(1, q_all, q_all)

    @pl.when(helps)
    def _():
        give_p.start()

    stream_rest(0)

    @pl.when(helps)
    def _():
        give_p.wait_send()
        give_q.wait_recv()

    @pl.when(leads)
    def _():
        give_p.wait_recv()
        copies = far_copies(0, lambda b: p_tx.at[b], p_rx.at[a])
        start(copies)
        stream(1, everyone, next(feeds))
        p_rx[a] = p_tx[a]
        wait(copies)
        total = p_rx[0]
        for i in range(1, SECTIONS):
            total = total + p_rx[i]
        q_tx[:, 0:half, :] = total.astype(BF16)
        q_all[c, a, :, 0:half, :] = total.astype(BF16)

        copies = far_copies(1, lambda b: q_tx, q_all.at[c, a])
        start(copies)
        stream(1, everyone, next(feeds))
        wait(copies)

        copies = loc_copies(0, own_q, own_q)
        start(copies)
        stream(1, everyone, next(feeds))
        wait(copies)
        give_q.start()
        give_q.wait_send()

    rotated = HEADS + KV_HEADS
    loads[6].wait()
    low = lax.broadcasted_iota(jnp.int32, (1, HEAD_DIM), 1) < 64

    def halves_of(row):
        turned = pltpu.roll(row, 64, 1)
        return jnp.where(low, row, turned), jnp.where(low, turned, row)

    for b in range(seqs):
        cos_hi, sin_hi = halves_of(table[pl.ds(lengths[b] // 64, 1), :])
        cos_lo, sin_lo = halves_of(table[pl.ds(HIGH_ROWS + lengths[b] % 64, 1), :])
        cosine = cos_hi * cos_lo - sin_hi * sin_lo
        sine = sin_hi * cos_lo + cos_hi * sin_lo
        sine = jnp.where(low, -sine, sine)
        for j in range(2 * SECTIONS):
            rank = j // 2
            rows[b, j * half : (j + 1) * half, :] = q_all[rank // 2, 2 * b + j % 2, rank % 2][
                :half
            ].astype(F32)
        x = rows[b, :rotated, :]
        x = x * cosine + pltpu.roll(x, 64, 1) * sine
        rows[b, :rotated, :] = x.astype(BF16).astype(F32)

    for copy in loads[1:3]:
        copy.wait()
    groups = HEADS // KV_HEADS
    inverse = 1.0 / math.sqrt(HEAD_DIM)
    pos_count = k_v.shape[1]
    first = (2 * t + s) * pos_count

    def one_sequence(b, carry):
        position = first + lax.broadcasted_iota(jnp.int32, (groups, pos_count), 1)
        usable = position < lengths[b]
        lane = lax.broadcasted_iota(jnp.int32, (groups, HEAD_DIM), 1)
        stats = []
        for k in range(KV_HEADS):
            lanes = slice(k * HEAD_DIM, (k + 1) * HEAD_DIM)
            q = rows[b, k * groups : (k + 1) * groups, :].astype(BF16)
            scores = nt_dot(q, k_v[b, :, lanes]) * inverse
            top = jnp.max(jnp.where(usable, scores, -1e30), -1, keepdims=True)
            weights = jnp.exp(jnp.where(usable, scores - top, -1e30))
            total = jnp.sum(weights, -1, keepdims=True)
            mix = jnp.dot(weights.astype(BF16), v_v[b, :, lanes], preferred_element_type=F32)
            stat = jnp.where((lane & 16) == 0, top, total)
            stats.append(jnp.where((lane >> 5) == b, stat, carry[k]))
            for g in range(groups):
                state[g // 2, k, g % 2, pl.ds(b, 1), :] = mix[g : g + 1, :]
        return tuple(stats)

    nothing = jnp.zeros((groups, HEAD_DIM), F32)
    stats = lax.fori_loop(0, seqs, one_sequence, (nothing,) * KV_HEADS)
    for k in range(KV_HEADS):
        for g in range(groups):
            state[g // 2, k, g % 2, seqs : seqs + 1, :] = stats[k][g : g + 1, :]

    def put(ref, part):
        mix, best, total = part
        low16 = (lax.broadcasted_iota(jnp.int32, best.shape, 1) & 16) == 0
        ref[0:seqs, :] = mix
        ref[seqs : seqs + 1, :] = jnp.where(low16, best, total)[0:1, :]

    give_state = duo_copy(2, state, a_rx1)
    give_head = duo_copy(3, heads.at[0], heads.at[0])

    @pl.when(helps)
    def _():
        give_state.start()
        give_state.wait_send()
        give_head.wait_recv()

    @pl.when(leads)
    def _():
        give_state.wait_recv()

        def merge_duo(i, carry):
            u, v = i // SECTIONS, i % SECTIONS
            for e in range(2):
                put(a_tx.at[u, v, e], merged([state[u, v, e], a_rx1[u, v, e]], seqs))
            return carry

        lax.fori_loop(0, NEAR * SECTIONS, merge_duo, 0, unroll=2)

        copies = loc_copies(
            1,
            lambda place, h: part_of(a_tx.at[place], 0, SECTIONS, h),
            lambda i, h: part_of(a_rx2.at[i], 0, SECTIONS, h),
        )
        start(copies)
        stream(1, everyone, next(feeds))
        a_rx2[3] = a_tx[c]
        wait(copies)

        def merge_loc(v, carry):
            for e in range(2):
                put(state.at[0, v, e], merged([a_rx2[i, v, e] for i in range(NEAR)], seqs))
            return carry

        lax.fori_loop(0, SECTIONS, merge_loc, 0)

        copies = far_copies(2, lambda b: state.at[0, b], a_rx3.at[a])
        start(copies)
        stream(1, everyone, next(feeds))
        a_rx3[a] = state[0, a]
        wait(copies)

        def head_rows(at):
            return jnp.concatenate([rows[b, pl.ds(at, 1), :] for b in range(seqs)], 0)

        for e in range(2):
            mix, best, total = merged([a_rx3[i, e] for i in range(SECTIONS)], seqs)
            best, total = spread(best), spread(total)
            head = groups * a + 2 * c + e
            products = head_rows(head) * head_rows(HEADS + a)
            own_score = jnp.sum(products, -1, keepdims=True) * inverse
            highest = jnp.maximum(best, own_score)
            old_scale = jnp.exp(best - highest)
            own_weight = jnp.exp(own_score - highest)
            numerator = mix * old_scale + own_weight * head_rows(rotated + a)
            denominator = total * old_scale + own_weight
            heads[e] = (numerator / denominator).astype(BF16).astype(F32)
        give_head.start()
        give_head.wait_send()

    loads[3].wait()
    attended = heads[s].astype(BF16)
    wide = 512
    for i in range(width // wide):
        y = jnp.dot(attended, wo_v[:, i * wide : (i + 1) * wide], preferred_element_type=F32)
        for j in range(wide // 128):
            part[i * (wide // 128) + j] = y[:, j * 128 : (j + 1) * 128]

    give_part = duo_copy(4, part, o_rx1)
    give_out = duo_copy(5, g_all, g_all)
    quarter = part.shape[0] // NEAR

    @pl.when(helps)
    def _():
        give_part.start()
        give_part.wait_send()
        give_out.wait_recv()

    @pl.when(leads)
    def _():
        give_part.wait_recv()
        part[...] = part[...] + o_rx1[...]
        copies = loc_copies(
            2,
            lambda place, h: part_of(part, place * quarter, quarter, h),
            lambda i, h: part_of(o_rx2.at[i], 0, quarter, h),
        )
        start(copies)
        stream(1, everyone, next(feeds))
        o_rx2[3] = part[pl.ds(c * quarter, quarter)]
        wait(copies)
        o_tx[...] = (o_rx2[0] + o_rx2[1]) + (o_rx2[2] + o_rx2[3])

        copies = far_copies(3, lambda b: o_tx.at[pl.ds(2 * b, 2)], o_rx3.at[a])
        start(copies)
        stream(1, everyone, next(feeds))
        o_rx3[a] = o_tx[pl.ds(2 * a, 2)]
        wait(copies)
        total = o_rx3[0]
        for i in range(1, SECTIONS):
            total = total + o_rx3[i]
        for e in range(2):
            col = pl.multiple_of((c * quarter + 2 * a + e) * 128, 128)
            g_all[c, a, e] = (hid[:, pl.ds(col, 128)].astype(F32) + total[e]).astype(BF16)

        copies = far_copies(4, lambda b: g_all.at[c, a], g_all.at[c, a])
        start(copies)
        stream(1, everyone, next(feeds))
        wait(copies)

        copies = loc_copies(3, own_g, own_g)
        start(copies)

    stream_rest(1)

    @pl.when(leads)
    def _():
        wait(loc_copies(3, own_g, own_g))
        give_out.start()
        give_out.wait_send()

    keep.wait()
    for k in everyone:
        piece(k, 0, cols).wait()


def place_kernel(order, recv, g_in, mixed, new, mixed_v, out_sem):
    per_section = ROW_BLOCKS // SECTIONS
    block = recv.shape[2] // per_section
    writes = []
    for i in range(ROW_BLOCKS):
        at = pl.multiple_of(order[i] * block, 128)
        src = recv.at[i // per_section, :, pl.ds((i % per_section) * block, block)]
        copy = pltpu.make_async_copy(src, new.at[:, pl.ds(at, block)], out_sem.at[i])
        copy.start()
        writes.append(copy)
    blocks = g_in.shape[0] * g_in.shape[1] * g_in.shape[2]
    for j in range(blocks):
        mixed_v[:, j * 128 : (j + 1) * 128] = g_in[
            j // (2 * SECTIONS), (j // 2) % SECTIONS, j % 2
        ]
    copy = pltpu.make_async_copy(mixed_v, mixed, out_sem.at[ROW_BLOCKS])
    copy.start()
    writes.append(copy)
    for copy in writes:
        copy.wait()


def turn_table():
    half_dim = HEAD_DIM // 2
    freqs = 500000.0 ** (-np.arange(half_dim) * 2.0 / HEAD_DIM)
    steps = np.concatenate([64 * np.arange(HIGH_ROWS), np.arange(64)])
    angles = steps[:, None] * freqs[None, :]
    return np.concatenate([np.cos(angles), np.sin(angles)], -1).astype(np.float32)


def shards(hidden_in, norm_gain, wqkv_old, wo, key_cache, value_cache, lengths, section_order):
    seqs, width = hidden_in.shape
    _, _, rank_cols, rows_old = wqkv_old.shape
    cols = rank_cols // SECTIONS
    block = width // ROW_BLOCKS
    pos_count = key_cache.shape[1]

    vmem = pl.BlockSpec(memory_space=pltpu.VMEM)
    smem = pl.BlockSpec(memory_space=pltpu.SMEM)
    hbm = pl.BlockSpec(memory_space=pl.ANY)
    dma = pltpu.SemaphoreType.DMA
    tile, five = (8, 128), (seqs + 1, 128)
    recv, blocks = pl.pallas_call(
        main_kernel,
        name="stream_and_decode",
        out_shape=(
            pltpu.VMEM((SECTIONS, cols, rows_old), BF16),
            pltpu.VMEM((NEAR, SECTIONS, 2, seqs, 128), BF16),
        ),
        in_specs=[hbm, hbm, hbm, smem, smem, hbm, hbm, hbm, hbm],
        out_specs=(vmem, vmem),
        scratch_shapes=[
            pltpu.VMEM((seqs, width), BF16),
            pltpu.VMEM((1, width), F32),
            pltpu.VMEM((HIGH_ROWS + 64, HEAD_DIM), F32),
            pltpu.VMEM((rank_cols, rows_old), BF16),
            pltpu.VMEM(wo.shape, BF16),
            pltpu.VMEM(key_cache.shape, BF16),
            pltpu.VMEM(value_cache.shape, BF16),
            pltpu.VMEM((ROW_BLOCKS, seqs, block), F32),
            pltpu.VMEM((SECTIONS, 2, *five), F32),
            pltpu.VMEM((SECTIONS, 2, *five), F32),
            pltpu.VMEM((2, *tile), BF16),
            pltpu.VMEM((NEAR, SECTIONS, 2, *tile), BF16),
            pltpu.VMEM((seqs, HEADS + 2 * KV_HEADS, HEAD_DIM), F32),
            pltpu.VMEM((NEAR, SECTIONS, 2, *five), F32),
            pltpu.VMEM((NEAR, SECTIONS, 2, *five), F32),
            pltpu.VMEM((NEAR, SECTIONS, 2, *five), F32),
            pltpu.VMEM((NEAR, SECTIONS, 2, *five), F32),
            pltpu.VMEM((SECTIONS, 2, *five), F32),
            pltpu.VMEM((2, seqs, HEAD_DIM), F32),
            pltpu.VMEM((width // 128, seqs, 128), F32),
            pltpu.VMEM((width // 128, seqs, 128), F32),
            pltpu.VMEM((NEAR, width // 512, seqs, 128), F32),
            pltpu.VMEM((width // 512, seqs, 128), F32),
            pltpu.VMEM((SECTIONS, 2, seqs, 128), F32),
            dma((8,)),
            dma((SECTIONS,)),
            dma((SECTIONS,)),
            dma((5, SECTIONS)),
            dma((5, SECTIONS)),
            dma((4, NEAR)),
            dma((4, NEAR)),
            dma((6,)),
            dma((6,)),
            pltpu.SemaphoreType.REGULAR((3,)),
            pltpu.SemaphoreType.REGULAR((3,)),
        ],
        compiler_params=pltpu.CompilerParams(collective_id=0, has_side_effects=True),
    )(
        hidden_in,
        norm_gain.reshape(1, width),
        jnp.asarray(turn_table()),
        lengths,
        section_order,
        wqkv_old.reshape(rank_cols, rows_old),
        wo,
        key_cache,
        value_cache,
    )

    mixed_out, new_weight = pl.pallas_call(
        place_kernel,
        name="place",
        out_shape=(
            jax.ShapeDtypeStruct((seqs, width), BF16),
            jax.ShapeDtypeStruct((cols, width), BF16),
        ),
        in_specs=[smem, vmem, vmem],
        out_specs=(hbm, hbm),
        scratch_shapes=[pltpu.VMEM((seqs, width), BF16), dma((ROW_BLOCKS + 1,))],
    )(
        section_order,
        pltpu.with_memory_space_constraint(recv, pltpu.VMEM),
        pltpu.with_memory_space_constraint(blocks, pltpu.VMEM),
    )
    return mixed_out, new_weight[None, None]


def solution(mesh):
    placed = (
        P("replica", None),
        P("replica"),
        P(("replica", "tp"), "sub", None, None),
        P(("replica", "tp", "sub"), None),
        P("replica", ("tp", "sub"), None),
        P("replica", ("tp", "sub"), None),
        P("replica"),
        P("replica"),
    )
    return jax.shard_map(
        shards,
        mesh=mesh,
        in_specs=placed,
        out_specs=(P("replica", None), P(("replica", "tp"), "sub", None, None)),
        check_vma=False,
    )
```

```python
import functools
import math

import jax
import jax.numpy as jnp
import numpy as np
from jax import lax
from jax.experimental import pallas as pl
from jax.experimental.pallas import tpu as pltpu
from jax.sharding import PartitionSpec as P

HEADS = 64
KV_HEADS = 8
HEAD_DIM = 128
ROW_BLOCKS = 16
NEAR = 4
SECTIONS = 8
FEEDS = (0, 0, 0, 1, 1, 1, 1, 1)
HIGH_ROWS = 72
STEP_ROWS = 16

FIRST = (4, 2, 1, 0)
MESH = pl.DeviceIdType.MESH
F32 = jnp.float32
BF16 = jnp.bfloat16


def nt_dot(x, y):
    return lax.dot_general(x, y, (((1,), (1,)), ((), ())), preferred_element_type=F32)


def spread(x):
    lane = lax.broadcasted_iota(jnp.int32, x.shape, 1)
    row = lax.broadcasted_iota(jnp.int32, x.shape, 0)
    return jnp.max(jnp.where((lane >> 5) == row, x, -3e38), -1, keepdims=True)


def merged(tiles, seqs):
    tops, totals = [], []
    low = (lax.broadcasted_iota(jnp.int32, (seqs, 128), 1) & 16) == 0
    for tile in tiles:
        stat = jnp.broadcast_to(tile[seqs : seqs + 1, :], (seqs, 128))
        tops.append(jnp.where(low, stat, pltpu.roll(stat, 16, 1)))
        totals.append(jnp.where(low, pltpu.roll(stat, 112, 1), stat))
    best = functools.reduce(jnp.maximum, tops)
    mix, total = None, None
    for tile, top, s in zip(tiles, tops, totals):
        f = jnp.exp(top - best)
        m = tile[0:seqs, :] * spread(f)
        mix = m if mix is None else mix + m
        total = s * f if total is None else total + s * f
    return mix, best, total


def main_kernel(
    hid_in, gain_in, table_in, lengths, order, w, wo, kc, vc,
    recv, g_all,
    hid, gain, table, w_v, wo_v, k_v, v_v, nrm, p_tx, p_rx, q_tx, q_all, rows, state, a_rx1, a_rx2,
    a_tx, a_rx3, heads, part, o_rx1, o_rx2, o_tx, o_rx3,
    load_sem, big_s, big_r, far_s, far_r, loc_s, loc_r, duo_s, duo_r, known_lo, known_hi,
):
    count = lax.axis_size("tp")
    t = lax.axis_index("tp")
    s = lax.axis_index("sub")
    a = t // NEAR
    c = t % NEAR
    seqs, width = hid_in.shape
    cols = recv.shape[1]
    leads, helps = s == 1, s == 0

    def far_id(k):
        return {"tp": lax.rem(t + NEAR * k, count)}

    def loc_id(d):
        return {"tp": lax.rem(t + d + count, count)}

    duo_id = {"sub": 1 - s}

    barrier = pltpu.get_barrier_semaphore()
    greeted = [loc_id(d) for d in (1, -1, 2, -2, NEAR, -NEAR)] + [duo_id]
    for target in greeted:
        pl.semaphore_signal(barrier, inc=1, device_id=target, device_id_type=MESH)

    loads = [
        pltpu.make_async_copy(src, dst, load_sem.at[i])
        for i, (src, dst) in enumerate(
            (
                (w, w_v),
                (kc, k_v),
                (vc, v_v),
                (wo, wo_v),
                (hid_in, hid),
                (gain_in, gain),
                (table_in, table),
            )
        )
    ]
    for i in (4, 5, 0):
        loads[i].start()
    pl.semaphore_wait(barrier, len(greeted))

    def piece(k, row, height):
        b = lax.rem(a + k, SECTIONS)
        first = pl.multiple_of(b * cols + row, 8)
        return pltpu.make_async_remote_copy(
            src_ref=w.at[pl.ds(first, height), :],
            dst_ref=recv.at[a, pl.ds(row, height), :],
            send_sem=big_s.at[k],
            recv_sem=big_r.at[SECTIONS - k],
            device_id=far_id(k),
            device_id_type=MESH,
        )

    sent = {}

    def stream(core, ks, n):
        ks = [k for k in ks if sent.get((core, k), 0) < cols]
        n = min([n] + [(cols - sent.get((core, k), 0)) // STEP_ROWS for k in ks])
        if not ks or n == 0:
            return
        starts = {k: sent.get((core, k), 0) for k in ks}

        def body(i, carry):
            for k in ks:
                piece(k, pl.multiple_of(starts[k] + i * STEP_ROWS, 8), STEP_ROWS).start()
            return carry

        @pl.when(s == core)
        def _():
            lax.fori_loop(0, n, body, 0)

        for k in ks:
            sent[core, k] = starts[k] + n * STEP_ROWS

    everyone = (4, 3, 5, 2, 6, 1, 7)
    feeds = iter(FEEDS)

    def stream_rest(core):
        stream(core, everyone[:5], cols // STEP_ROWS)
        while any(sent.get((core, k), 0) < cols for k in everyone):
            stream(core, everyone, cols // STEP_ROWS)

    def tell(stage):
        pl.semaphore_signal(known_lo.at[stage], inc=1, device_id=far_id(1), device_id_type=MESH)
        pl.semaphore_signal(
            known_hi.at[stage], inc=1, device_id=far_id(SECTIONS - 1), device_id_type=MESH
        )

    def hear(stage):
        pl.semaphore_wait(known_lo.at[stage], 1)
        pl.semaphore_wait(known_hi.at[stage], 1)

    tell(0)
    stream(0, (1, 7), FIRST[0])
    stream(1, (1, 7), FIRST[3])
    for i in (6, 1, 2, 3):
        loads[i].start()
    hear(0)
    tell(1)
    stream(0, (2, 6), FIRST[1])

    def remote(src, dst, send_sem, recv_sem, target):
        return pltpu.make_async_remote_copy(
            src_ref=src,
            dst_ref=dst,
            send_sem=send_sem,
            recv_sem=recv_sem,
            device_id=target,
            device_id_type=MESH,
        )

    def far_copies(phase, src, dst):
        return [
            remote(
                src(lax.rem(a + k, SECTIONS)),
                dst,
                far_s.at[phase, k],
                far_r.at[phase, SECTIONS - k],
                far_id(k),
            )
            for k in (4, 3, 5, 2, 6, 1, 7)
        ]

    def loc_copies(phase, src, dst):
        out = []
        for i, (d, h) in enumerate(((1, None), (-1, None), (2, 0), (-2, 1))):
            place = lax.rem(c + d + NEAR, NEAR)
            sems = loc_s.at[phase, i], loc_r.at[phase, i]
            out.append(remote(src(place, h), dst(min(i, 2), h), *sems, loc_id(d)))
        return out

    def part_of(ref, at, size, h):
        if h is None:
            return ref.at[pl.ds(at, size)]
        return ref.at[pl.ds(at + h * (size // 2), size // 2)]

    def duo_copy(phase, src, dst):
        return remote(src, dst, duo_s.at[phase], duo_r.at[phase], duo_id)

    def start(copies):
        for copy in copies:
            copy.start()

    def wait(copies):
        for copy in copies:
            copy.wait()

    loads[4].wait()
    loads[5].wait()
    block = nrm.shape[2]
    squares = jnp.zeros((seqs, 1), F32)
    for i in range(ROW_BLOCKS):
        x = hid[:, i * block : (i + 1) * block].astype(F32)
        squares = squares + jnp.sum(x * x, -1, keepdims=True)
    factor = lax.rsqrt(squares * (1.0 / width) + 1e-05)
    for i in range(ROW_BLOCKS):
        x = hid[:, i * block : (i + 1) * block].astype(F32)
        y = (x * factor * gain[:, i * block : (i + 1) * block]).astype(BF16)
        nrm[i] = y.astype(F32)

    hear(1)
    tell(2)
    stream(0, (3, 5), FIRST[2])

    per_section = ROW_BLOCKS // SECTIONS
    mine = [nrm[order[per_section * a + i]].astype(BF16) for i in range(per_section)]
    normed = jnp.concatenate(mine, -1)
    loads[0].wait()
    units = w.shape[0] // HEAD_DIM
    half = units // 2
    for u in range(units):
        y = nt_dot(normed, w_v[u * HEAD_DIM : (u + 1) * HEAD_DIM, :])
        for b in range(seqs):
            p_tx[2 * b + u // half, s, u % half : u % half + 1, :] = y[b : b + 1, :]
    own_rows = pl.ds(pl.multiple_of(a * cols, 8), cols)
    keep = pltpu.make_async_copy(w.at[own_rows, :], recv.at[a], load_sem.at[7])
    keep.start()

    hear(2)
    def own_q(_, h):
        return part_of(q_all.at[c], 0, SECTIONS, h)

    def own_g(_, h):
        return part_of(g_all.at[c], 0, SECTIONS, h)

    give_p = duo_copy(0, p_tx.at[:, 0], p_tx.at[:, 0])
    give_q = duo_copy(1, q_all, q_all)

    @pl.when(helps)
    def _():
        give_p.start()

    stream_rest(0)

    @pl.when(helps)
    def _():
        give_p.wait_send()
        give_q.wait_recv()

    @pl.when(leads)
    def _():
        give_p.wait_recv()
        copies = far_copies(0, lambda b: p_tx.at[b], p_rx.at[a])
        start(copies)
        stream(1, everyone, next(feeds))
        p_rx[a] = p_tx[a]
        wait(copies)
        total = p_rx[0]
        for i in range(1, SECTIONS):
            total = total + p_rx[i]
        q_tx[:, 0:half, :] = total.astype(BF16)
        q_all[c, a, :, 0:half, :] = total.astype(BF16)

        copies = far_copies(1, lambda b: q_tx, q_all.at[c, a])
        start(copies)
        stream(1, everyone, next(feeds))
        wait(copies)

        copies = loc_copies(0, own_q, own_q)
        start(copies)
        stream(1, everyone, next(feeds))
        wait(copies)
        give_q.start()
        give_q.wait_send()

    rotated = HEADS + KV_HEADS
    loads[6].wait()
    low = lax.broadcasted_iota(jnp.int32, (1, HEAD_DIM), 1) < 64

    def halves_of(row):
        turned = pltpu.roll(row, 64, 1)
        return jnp.where(low, row, turned), jnp.where(low, turned, row)

    for b in range(seqs):
        cos_hi, sin_hi = halves_of(table[pl.ds(lengths[b] // 64, 1), :])
        cos_lo, sin_lo = halves_of(table[pl.ds(HIGH_ROWS + lengths[b] % 64, 1), :])
        cosine = cos_hi * cos_lo - sin_hi * sin_lo
        sine = sin_hi * cos_lo + cos_hi * sin_lo
        sine = jnp.where(low, -sine, sine)
        for j in range(2 * SECTIONS):
            rank = j // 2
            rows[b, j * half : (j + 1) * half, :] = q_all[rank // 2, 2 * b + j % 2, rank % 2][
                :half
            ].astype(F32)
        x = rows[b, :rotated, :]
        x = x * cosine + pltpu.roll(x, 64, 1) * sine
        rows[b, :rotated, :] = x.astype(BF16).astype(F32)

    for copy in loads[1:3]:
        copy.wait()
    groups = HEADS // KV_HEADS
    inverse = 1.0 / math.sqrt(HEAD_DIM)
    pos_count = k_v.shape[1]
    first = (2 * t + s) * pos_count

    def one_sequence(b, carry):
        position = first + lax.broadcasted_iota(jnp.int32, (groups, pos_count), 1)
        usable = position < lengths[b]
        lane = lax.broadcasted_iota(jnp.int32, (groups, HEAD_DIM), 1)
        stats = []
        for k in range(KV_HEADS):
            lanes = slice(k * HEAD_DIM, (k + 1) * HEAD_DIM)
            q = rows[b, k * groups : (k + 1) * groups, :].astype(BF16)
            scores = nt_dot(q, k_v[b, :, lanes]) * inverse
            top = jnp.max(jnp.where(usable, scores, -1e30), -1, keepdims=True)
            weights = jnp.exp(jnp.where(usable, scores - top, -1e30))
            total = jnp.sum(weights, -1, keepdims=True)
            mix = jnp.dot(weights.astype(BF16), v_v[b, :, lanes], preferred_element_type=F32)
            stat = jnp.where((lane & 16) == 0, top, total)
            stats.append(jnp.where((lane >> 5) == b, stat, carry[k]))
            for g in range(groups):
                state[g // 2, k, g % 2, pl.ds(b, 1), :] = mix[g : g + 1, :]
        return tuple(stats)

    nothing = jnp.zeros((groups, HEAD_DIM), F32)
    stats = lax.fori_loop(0, seqs, one_sequence, (nothing,) * KV_HEADS)
    for k in range(KV_HEADS):
        for g in range(groups):
            state[g // 2, k, g % 2, seqs : seqs + 1, :] = stats[k][g : g + 1, :]

    def put(ref, part):
        mix, best, total = part
        low16 = (lax.broadcasted_iota(jnp.int32, best.shape, 1) & 16) == 0
        ref[0:seqs, :] = mix
        ref[seqs : seqs + 1, :] = jnp.where(low16, best, total)[0:1, :]

    give_state = duo_copy(2, state, a_rx1)
    give_head = duo_copy(3, heads.at[0], heads.at[0])

    @pl.when(helps)
    def _():
        give_state.start()
        give_state.wait_send()
        give_head.wait_recv()

    @pl.when(leads)
    def _():
        give_state.wait_recv()

        def merge_duo(i, carry):
            u, v = i // SECTIONS, i % SECTIONS
            for e in range(2):
                put(a_tx.at[u, v, e], merged([state[u, v, e], a_rx1[u, v, e]], seqs))
            return carry

        lax.fori_loop(0, NEAR * SECTIONS, merge_duo, 0, unroll=2)

        copies = loc_copies(
            1,
            lambda place, h: part_of(a_tx.at[place], 0, SECTIONS, h),
            lambda i, h: part_of(a_rx2.at[i], 0, SECTIONS, h),
        )
        start(copies)
        stream(1, everyone, next(feeds))
        a_rx2[3] = a_tx[c]
        wait(copies)

        def merge_loc(v, carry):
            for e in range(2):
                put(state.at[0, v, e], merged([a_rx2[i, v, e] for i in range(NEAR)], seqs))
            return carry

        lax.fori_loop(0, SECTIONS, merge_loc, 0)

        copies = far_copies(2, lambda b: state.at[0, b], a_rx3.at[a])
        start(copies)
        stream(1, everyone, next(feeds))
        a_rx3[a] = state[0, a]
        wait(copies)

        def head_rows(at):
            return jnp.concatenate([rows[b, pl.ds(at, 1), :] for b in range(seqs)], 0)

        for e in range(2):
            mix, best, total = merged([a_rx3[i, e] for i in range(SECTIONS)], seqs)
            best, total = spread(best), spread(total)
            head = groups * a + 2 * c + e
            products = head_rows(head) * head_rows(HEADS + a)
            own_score = jnp.sum(products, -1, keepdims=True) * inverse
            highest = jnp.maximum(best, own_score)
            old_scale = jnp.exp(best - highest)
            own_weight = jnp.exp(own_score - highest)
            numerator = mix * old_scale + own_weight * head_rows(rotated + a)
            denominator = total * old_scale + own_weight
            heads[e] = (numerator / denominator).astype(BF16).astype(F32)
        give_head.start()
        give_head.wait_send()

    loads[3].wait()
    attended = heads[s].astype(BF16)
    wide = 512
    for i in range(width // wide):
        y = jnp.dot(attended, wo_v[:, i * wide : (i + 1) * wide], preferred_element_type=F32)
        for j in range(wide // 128):
            part[i * (wide // 128) + j] = y[:, j * 128 : (j + 1) * 128]

    give_part = duo_copy(4, part, o_rx1)
    give_out = duo_copy(5, g_all, g_all)
    quarter = part.shape[0] // NEAR

    @pl.when(helps)
    def _():
        give_part.start()
        give_part.wait_send()
        give_out.wait_recv()

    @pl.when(leads)
    def _():
        give_part.wait_recv()
        part[...] = part[...] + o_rx1[...]
        copies = loc_copies(
            2,
            lambda place, h: part_of(part, place * quarter, quarter, h),
            lambda i, h: part_of(o_rx2.at[i], 0, quarter, h),
        )
        start(copies)
        stream(1, everyone, next(feeds))
        o_rx2[3] = part[pl.ds(c * quarter, quarter)]
        wait(copies)
        o_tx[...] = (o_rx2[0] + o_rx2[1]) + (o_rx2[2] + o_rx2[3])

        copies = far_copies(3, lambda b: o_tx.at[pl.ds(2 * b, 2)], o_rx3.at[a])
        start(copies)
        stream(1, everyone, next(feeds))
        o_rx3[a] = o_tx[pl.ds(2 * a, 2)]
        wait(copies)
        total = o_rx3[0]
        for i in range(1, SECTIONS):
            total = total + o_rx3[i]
        for e in range(2):
            col = pl.multiple_of((c * quarter + 2 * a + e) * 128, 128)
            g_all[c, a, e] = (hid[:, pl.ds(col, 128)].astype(F32) + total[e]).astype(BF16)

        copies = far_copies(4, lambda b: g_all.at[c, a], g_all.at[c, a])
        start(copies)
        stream(1, everyone, next(feeds))
        wait(copies)

        copies = loc_copies(3, own_g, own_g)
        start(copies)

    stream_rest(1)

    @pl.when(leads)
    def _():
        wait(loc_copies(3, own_g, own_g))
        give_out.start()
        give_out.wait_send()

    keep.wait()
    for k in everyone:
        piece(k, 0, cols).wait()


def place_kernel(order, recv, g_in, mixed, new, mixed_v, out_sem):
    per_section = ROW_BLOCKS // SECTIONS
    block = recv.shape[2] // per_section
    writes = []
    for i in range(ROW_BLOCKS):
        at = pl.multiple_of(order[i] * block, 128)
        src = recv.at[i // per_section, :, pl.ds((i % per_section) * block, block)]
        copy = pltpu.make_async_copy(src, new.at[:, pl.ds(at, block)], out_sem.at[i])
        copy.start()
        writes.append(copy)
    blocks = g_in.shape[0] * g_in.shape[1] * g_in.shape[2]
    for j in range(blocks):
        mixed_v[:, j * 128 : (j + 1) * 128] = g_in[
            j // (2 * SECTIONS), (j // 2) % SECTIONS, j % 2
        ]
    copy = pltpu.make_async_copy(mixed_v, mixed, out_sem.at[ROW_BLOCKS])
    copy.start()
    writes.append(copy)
    for copy in writes:
        copy.wait()


def turn_table():
    half_dim = HEAD_DIM // 2
    freqs = 500000.0 ** (-np.arange(half_dim) * 2.0 / HEAD_DIM)
    steps = np.concatenate([64 * np.arange(HIGH_ROWS), np.arange(64)])
    angles = steps[:, None] * freqs[None, :]
    return np.concatenate([np.cos(angles), np.sin(angles)], -1).astype(np.float32)


def shards(hidden_in, norm_gain, wqkv_old, wo, key_cache, value_cache, lengths, section_order):
    seqs, width = hidden_in.shape
    _, _, rank_cols, rows_old = wqkv_old.shape
    cols = rank_cols // SECTIONS
    block = width // ROW_BLOCKS
    pos_count = key_cache.shape[1]

    vmem = pl.BlockSpec(memory_space=pltpu.VMEM)
    smem = pl.BlockSpec(memory_space=pltpu.SMEM)
    hbm = pl.BlockSpec(memory_space=pl.ANY)
    dma = pltpu.SemaphoreType.DMA
    tile, five = (8, 128), (seqs + 1, 128)
    recv, blocks = pl.pallas_call(
        main_kernel,
        name="stream_and_decode",
        out_shape=(
            pltpu.VMEM((SECTIONS, cols, rows_old), BF16),
            pltpu.VMEM((NEAR, SECTIONS, 2, seqs, 128), BF16),
        ),
        in_specs=[hbm, hbm, hbm, smem, smem, hbm, hbm, hbm, hbm],
        out_specs=(vmem, vmem),
        scratch_shapes=[
            pltpu.VMEM((seqs, width), BF16),
            pltpu.VMEM((1, width), F32),
            pltpu.VMEM((HIGH_ROWS + 64, HEAD_DIM), F32),
            pltpu.VMEM((rank_cols, rows_old), BF16),
            pltpu.VMEM(wo.shape, BF16),
            pltpu.VMEM(key_cache.shape, BF16),
            pltpu.VMEM(value_cache.shape, BF16),
            pltpu.VMEM((ROW_BLOCKS, seqs, block), F32),
            pltpu.VMEM((SECTIONS, 2, *five), F32),
            pltpu.VMEM((SECTIONS, 2, *five), F32),
            pltpu.VMEM((2, *tile), BF16),
            pltpu.VMEM((NEAR, SECTIONS, 2, *tile), BF16),
            pltpu.VMEM((seqs, HEADS + 2 * KV_HEADS, HEAD_DIM), F32),
            pltpu.VMEM((NEAR, SECTIONS, 2, *five), F32),
            pltpu.VMEM((NEAR, SECTIONS, 2, *five), F32),
            pltpu.VMEM((NEAR, SECTIONS, 2, *five), F32),
            pltpu.VMEM((NEAR, SECTIONS, 2, *five), F32),
            pltpu.VMEM((SECTIONS, 2, *five), F32),
            pltpu.VMEM((2, seqs, HEAD_DIM), F32),
            pltpu.VMEM((width // 128, seqs, 128), F32),
            pltpu.VMEM((width // 128, seqs, 128), F32),
            pltpu.VMEM((NEAR, width // 512, seqs, 128), F32),
            pltpu.VMEM((width // 512, seqs, 128), F32),
            pltpu.VMEM((SECTIONS, 2, seqs, 128), F32),
            dma((8,)),
            dma((SECTIONS,)),
            dma((SECTIONS,)),
            dma((5, SECTIONS)),
            dma((5, SECTIONS)),
            dma((4, NEAR)),
            dma((4, NEAR)),
            dma((6,)),
            dma((6,)),
            pltpu.SemaphoreType.REGULAR((3,)),
            pltpu.SemaphoreType.REGULAR((3,)),
        ],
        compiler_params=pltpu.CompilerParams(collective_id=0, has_side_effects=True),
    )(
        hidden_in,
        norm_gain.reshape(1, width),
        jnp.asarray(turn_table()),
        lengths,
        section_order,
        wqkv_old.reshape(rank_cols, rows_old),
        wo,
        key_cache,
        value_cache,
    )

    mixed_out, new_weight = pl.pallas_call(
        place_kernel,
        name="place",
        out_shape=(
            jax.ShapeDtypeStruct((seqs, width), BF16),
            jax.ShapeDtypeStruct((cols, width), BF16),
        ),
        in_specs=[smem, vmem, vmem],
        out_specs=(hbm, hbm),
        scratch_shapes=[pltpu.VMEM((seqs, width), BF16), dma((ROW_BLOCKS + 1,))],
    )(
        section_order,
        pltpu.with_memory_space_constraint(recv, pltpu.VMEM),
        pltpu.with_memory_space_constraint(blocks, pltpu.VMEM),
    )
    return mixed_out, new_weight[None, None]


def solution(mesh):
    placed = (
        P("replica", None),
        P("replica"),
        P(("replica", "tp"), "sub", None, None),
        P(("replica", "tp", "sub"), None),
        P("replica", ("tp", "sub"), None),
        P("replica", ("tp", "sub"), None),
        P("replica"),
        P("replica"),
    )
    return jax.shard_map(
        shards,
        mesh=mesh,
        in_specs=placed,
        out_specs=(P("replica", None), P(("replica", "tp"), "sub", None, None)),
        check_vma=False,
    )
```
